32 devices in a mesh: dom: 8 (over y, x, core), band: 4 (over z).
Axes of the slice: x: 2, y: 2, z: 4, core: 2. Of those that a mesh axis runs over, the one named last changes fastest.
Arguments:
- orbitals: bfloat16 [768, 8, 6, 1152], P('band', 'dom'), may hold values from -6 to 6
- occupations: float32 [768], P('band'), may hold values from 0.2 to 2
- previous: float32 [8, 12, 4608], P('dom'), may hold values from -6 to 6
- compensation: float32 [8, 12, 4608], P('dom'), may hold values from 0 to 1.5
- local_potential: float32 [8, 6, 1152], P('dom'), may hold values from -6 to 6
Outputs:
- applied: bfloat16 [768, 8, 6, 1152], P('band', 'dom')
- potential: float32 [8, 12, 4608], P('dom')
The draws below stay inside these ranges and needn't reach their ends.
All inputs are finite; a program needn't handle non-finite values.
Results may differ from the reference program's by a relative error of at most 0.001.
Values may be sent and summed in bfloat16 or wider, within the bound.
No kernel may reach another device: no remote copies, remote signals or barrier semaphores. Data moves between devices by JAX's collectives and lax.ppermute only.
A program may use at most 64 MiB of HBM per device.

```python
import math
import jax
import jax.numpy as jnp
from jax import lax

BANDS = 768
BX = 6
BY = 24
BZ = 48
SWEEPS = 4
DZ = 2
DY = 2
DX = 2
N_DOM = 8


def block_scale(key, extent, pieces, least, high):
    gain, own = 1.0, jax.random.fold_in(key, 6)
    for position, blocks in pieces:
        heights = jnp.exp(jax.random.uniform(jax.random.fold_in(own, position), (blocks,), jnp.float32, least / len(pieces), high / len(pieces)))
        gain = gain * jnp.repeat(heights, extent[position] // blocks).reshape([-1 if axis == position else 1 for axis in range(len(extent))])
    return gain


def normal_values(own_key, shape, deviation, bound, pieces=(), dtype=jnp.bfloat16):
    drawn = jax.random.normal(own_key, shape, jnp.float32) * deviation
    if len(pieces) > 0:
        drawn = block_scale(own_key, shape, pieces, -0.22, 0.18) * drawn
    return jnp.clip(drawn, min=-bound, max=bound).astype(dtype)


def setup_inputs(seed: int = 0) -> dict:
    splits = jax.random.split(jax.random.key(seed), 6)
    orbitals = normal_values(splits[0], (BANDS, N_DOM, BX, BY * BZ), 1.0, 6.0, ((0, 4), (1, 8)))
    occupations = jnp.clip(jnp.exp(math.log(2.0) - 2.3025851 * jax.random.uniform(splits[1], (BANDS,), jnp.float32) ** block_scale(splits[1], (BANDS,), ((0, 4),), -0.2, 0.2)), 0.2, 2.0)
    previous = normal_values(splits[2], (N_DOM, 2 * BX, 4 * BY * BZ), 1.0, 6.0, ((0, 8),), jnp.float32)
    compensation = jnp.clip(1.5 * jax.random.uniform(splits[3], (N_DOM, 2 * BX, 4 * BY * BZ), jnp.float32) ** block_scale(splits[3], (N_DOM, 2 * BX, 4 * BY * BZ), ((0, 8),), -0.2, 0.2), 0.0, 1.5)
    local_potential = normal_values(splits[4], (N_DOM, BX, BY * BZ), 1.0, 6.0, ((0, 8),), jnp.float32)
    return dict(orbitals=orbitals, occupations=occupations, previous=previous, compensation=compensation, local_potential=local_potential)


precise = lax.Precision.HIGHEST


def to_grid(blocks, size_x, size_y, size_z):
    leading = blocks.shape[:-3]
    count = len(leading)
    shaped = blocks.reshape(leading + (DX, DY, DZ, size_x, size_y, size_z))
    permuted = tuple(range(count)) + (count, count + 3, count + 1, count + 4, count + 2, count + 5)
    return shaped.transpose(permuted).reshape(leading + (DX * size_x, DY * size_y, DZ * size_z))


def to_blocks(grid_field, size_x, size_y, size_z):
    leading = grid_field.shape[:-3]
    count = len(leading)
    shaped = grid_field.reshape(leading + (DX, size_x, DY, size_y, DZ, size_z))
    permuted = tuple(range(count)) + (count, count + 2, count + 4, count + 1, count + 3, count + 5)
    return shaped.transpose(permuted).reshape(leading + (DX * DY * DZ, size_x, size_y * size_z))


def pad_three(array_in):
    return jnp.pad(array_in, [(0, 0)] * (array_in.ndim - 3) + [(1, 1)] * 3)


def neighbour_sum(array_in):
    padded = pad_three(array_in)
    total = padded[..., 2:, 1:-1, 1:-1] + padded[..., :-2, 1:-1, 1:-1]
    total = total + padded[..., 1:-1, 2:, 1:-1] + padded[..., 1:-1, :-2, 1:-1]
    return total + padded[..., 1:-1, 1:-1, 2:] + padded[..., 1:-1, 1:-1, :-2]


def refine_axis(padded, along):
    front = jnp.moveaxis(padded, along, 0)
    middle = front[1:-1]
    even_rows = 0.75 * middle + 0.25 * front[:-2]
    odd_rows = 0.75 * middle + 0.25 * front[2:]
    refined = jnp.stack([even_rows, odd_rows], 1).reshape((2 * middle.shape[0],) + middle.shape[1:])
    return jnp.moveaxis(refined, 0, along)


def coarsen_axis(padded, along):
    front = jnp.moveaxis(padded, along, 0)
    half_rows = (front.shape[0] - 2) // 2
    middle = front[1:-1].reshape((half_rows, 2) + front.shape[1:])
    left_rows = front[0:2 * half_rows:2]
    right_rows = front[3:2 * half_rows + 2:2]
    coarse = 0.5 * (0.25 * left_rows + 0.75 * middle[:, 0] + 0.75 * middle[:, 1] + 0.25 * right_rows)
    return jnp.moveaxis(coarse, 0, along)


def reference(orbitals, occupations, previous, compensation, local_potential):
    group_size = math.gcd(BANDS, 32)
    orbital_groups = orbitals.reshape(BANDS // group_size, group_size, N_DOM, BX, BY * BZ)
    occupation_groups = occupations.reshape(BANDS // group_size, group_size)

    def accumulate(running, items):
        wave_field = items[0].astype(jnp.float32).reshape(group_size, N_DOM * BX * BY * BZ)
        return running + jnp.dot(items[1], wave_field * wave_field, precision=precise), None

    running, unused = lax.scan(accumulate, jnp.zeros((N_DOM * BX * BY * BZ,), jnp.float32), (orbital_groups, occupation_groups))
    density = to_grid((running / BANDS).reshape(N_DOM, BX, BY * BZ), BX, BY, BZ)
    refined = refine_axis(pad_three(density), 0)
    refined = refine_axis(refined, 1)
    refined = refine_axis(refined, 2)
    source = math.pi * (refined - to_grid(compensation, 2 * BX, 2 * BY, 2 * BZ))
    potential = to_grid(previous, 2 * BX, 2 * BY, 2 * BZ)
    for counter in range(SWEEPS):
        potential = (neighbour_sum(potential) + source) / 6.0
    coarse = coarsen_axis(pad_three(potential), 0)
    coarse = coarsen_axis(coarse, 1)
    coarse = coarsen_axis(coarse, 2)
    effective = coarse - jnp.cbrt(3.0 / math.pi * density) + to_grid(local_potential, BX, BY, BZ)
    effective_blocks = to_blocks(effective, BX, BY, BZ)

    def apply_group(group):
        wave_field = group.astype(jnp.float32)
        grid_field = to_grid(wave_field, BX, BY, BZ)
        laplace = to_blocks(neighbour_sum(grid_field) - 6.0 * grid_field, BX, BY, BZ)
        return (-0.5 * laplace + effective_blocks[None] * wave_field).astype(jnp.bfloat16)

    applied = lax.map(apply_group, orbital_groups).reshape(BANDS, N_DOM, BX, BY * BZ)
    return applied, to_blocks(potential, 2 * BX, 2 * BY, 2 * BZ)
```

```python
import functools
import math

import jax
import jax.numpy as jnp
import numpy as np
from jax import lax
from jax.experimental import pallas as pl
from jax.experimental.pallas import tpu as pltpu
from jax.sharding import PartitionSpec as P

BY = 24
BZ = 48
SWEEPS = 4

F32, BF16 = jnp.float32, jnp.bfloat16
LANES = 128
PAD = 8
ZOFF = 16
WV = SWEEPS + 1
WS = SWEEPS
WC = WS // 2 + 1


def sides(count):
    return ("swap",) if count == 2 else ("lo", "hi")


def fetch(block, counts, moves):
    pairs = []
    for target in np.ndindex(*counts):
        source = list(target)
        for axis, side in moves.items():
            source[axis] = {"swap": 1 - target[axis], "lo": target[axis] - 1, "hi": target[axis] + 1}[side]
        if all(0 <= s < n for s, n in zip(source, counts)):
            pairs.append((int(np.ravel_multi_index(source, counts)), int(np.ravel_multi_index(target, counts))))
    return lax.ppermute(block, "dom", pairs)


def rim_start(side, coord, length, width):
    if side == "swap":
        return jnp.where(coord == 0, length - width, 0)
    return length - width if side == "lo" else 0


def halo_start(side, coord, low, high):
    if side == "swap":
        return jnp.where(coord == 0, high, low)
    return low if side == "lo" else high


def lane_iota(rows):
    return lax.broadcasted_iota(jnp.int32, (rows, LANES), 1)


def exact_dot(value, weights):
    high = value.astype(BF16)
    rest = value - high.astype(F32)
    middle = rest.astype(BF16)
    low = (rest - middle.astype(F32)).astype(BF16)
    dot = functools.partial(jnp.dot, preferred_element_type=F32)
    return dot(high, weights) + (dot(middle, weights) + dot(low, weights))


def z_refine():
    w = np.zeros((2, LANES, LANES), np.float32)
    for c in range(2):
        for lane in range(LANES):
            fine = 2 * BZ * c + lane - ZOFF
            if 0 <= fine < 4 * BZ:
                cell = fine // 2
                other = cell + (1 if fine % 2 else -1)
                w[c, cell, lane] += 0.75
                if 0 <= other < 2 * BZ:
                    w[c, other, lane] += 0.25
    return w


def z_coarsen():
    w = np.zeros((LANES, LANES), np.float32)
    for cell in range(BZ):
        for step, value in ((-1, 0.125), (0, 0.375), (1, 0.375), (2, 0.125)):
            w[ZOFF + 2 * cell + step, cell] = value
    return w


def z_pick():
    w = np.zeros((2, BY * BZ, LANES), np.float32)
    for y in range(BY):
        w[0, y * BZ + BZ - 1, y] = 1
        w[1, y * BZ, y] = 1
    return w


def z_spread():
    w = np.zeros((2, LANES, BY * BZ), np.float32)
    for y in range(BY):
        w[0, y, y * BZ + BZ - 1] = 1
        w[1, y, y * BZ] = 1
    return w


def z_masks():
    z = np.arange(BY * BZ) % BZ
    w = np.zeros((8, BY * BZ), np.float32)
    w[0] = z != 0
    w[1] = z != BZ - 1
    return w


def density_kernel(counts, pos, orb, occ, pick, part, zf, *faces):
    x = pl.program_id(0)
    planes = pl.num_programs(0)
    tiles = orb.shape[2] // LANES
    x_sides, y_sides = sides(counts[0]), sides(counts[1])
    x_faces, y_faces = faces[: len(x_sides)], faces[len(x_sides) :]
    weight = jnp.broadcast_to(occ[...], (orb.shape[1], LANES))
    for t in range(tiles):
        f = orb[0, :, t * LANES : (t + 1) * LANES].astype(F32)
        part[pl.ds(tiles * x + t, 1), :] = jnp.sum(f * f * weight, axis=0, keepdims=True)
    zf[0] = jnp.dot(orb[0], pick[0], preferred_element_type=F32).astype(BF16)
    for side, face in zip(y_sides, y_faces):
        start = rim_start(side, pos[1], orb.shape[2], LANES)
        face[0] = orb[0, :, pl.ds(pl.multiple_of(start, LANES), LANES)]
    for side, face in zip(x_sides, x_faces):
        @pl.when(x == rim_start(side, pos[0], planes, 1))
        def _(face=face):
            face[...] = orb[0]


def total_kernel(scale, pos, *refs):
    parts, out, flat = refs[:-2], refs[-2], refs[-1]
    total = parts[0][...]
    for part in parts[1:]:
        total = total + part[...]
    flat[...] = total * scale
    per = 384 // BZ
    groups = flat.shape[0] // 3
    lane = lane_iota(groups)
    shift = jnp.where(pos[2] == 0, 0, BZ)
    tile = [flat[pl.ds(j, groups, stride=3), :] for j in range(3)]
    for k in range(per):
        at, off = divmod(BZ * k, LANES)
        row = pltpu.roll(tile[at], (LANES - off) % LANES, 1) if off else tile[at]
        if off + BZ > LANES:
            row = jnp.where(lane < LANES - off, row, pltpu.roll(tile[at + 1], LANES - off, 1))
        row = jnp.where(lane < BZ, row, 0.0)
        out[pl.ds(k, groups, stride=per), :] = pltpu.roll(row, shift, 1)


def field_rows(ref, groups):
    lane = lane_iota(groups)
    a, b, c = (ref[pl.ds(j, groups, stride=3), :] for j in range(3))
    return (
        pltpu.roll(a, 16, 1),
        jnp.where(lane < 48, pltpu.roll(a, 48, 1), pltpu.roll(b, 48, 1)),
        jnp.where(lane < 80, pltpu.roll(b, 80, 1), pltpu.roll(c, 80, 1)),
        pltpu.roll(c, 112, 1),
    )


def field_kernel(counts, pos, prev, comp, mate, ext, *refs):
    mate32, sends = refs[-1], list(refs[:-1])
    fx, fy = 2 * mate32.shape[0] * LANES // (2 * 2 * 2 * BY * 2 * BZ), 2 * BY
    groups = prev.shape[0] // 3
    lane = lane_iota(groups)
    own = (lane >= ZOFF) & (lane < ZOFF + 2 * BZ)
    first = pos[2] == 0
    shift = jnp.where(first, 2 * BZ, LANES - 2 * BZ)
    edge_low = jnp.where(first, ZOFF + 2 * BZ, 0)
    edge_high = jnp.where(first, LANES, ZOFF)
    edge = (lane >= edge_low) & (lane < edge_high)
    mate32[...] = mate[...].astype(F32)
    rows = fx * fy
    for f, ref in enumerate((prev, comp)):
        mine = field_rows(ref, groups)
        theirs = field_rows(mate32.at[pl.ds(f * prev.shape[0], prev.shape[0])], groups)
        for k in range(4):
            halo = jnp.where(edge, pltpu.roll(theirs[k], shift, 1), 0.0)
            ext[pl.ds(f * rows + k, groups, stride=4), :] = jnp.where(own, mine[k], halo)
    widths = (WV, WS)
    x_sides, y_sides = sides(counts[0]), sides(counts[1])
    for side in x_sides:
        send, done = sends.pop(0), 0
        for f, width in enumerate(widths):
            start = f * rows + fy * rim_start(side, pos[0], fx, width)
            send[pl.ds(done, width * fy), :] = ext[pl.ds(pl.multiple_of(start, 8), width * fy), :].astype(BF16)
            done += width * fy
    for side in y_sides:
        send = sends.pop(0)
        at = rim_start(side, pos[1], fy, PAD)
        for f in range(2):
            cut = [ext[pl.ds(pl.multiple_of(f * rows + fy * x + at, 8), PAD), :] for x in range(fx)]
            send[pl.ds(f * fx * PAD, fx * PAD), :] = jnp.concatenate(cut, 0).astype(BF16)
    for x_side in x_sides:
        for y_side in y_sides:
            send = sends.pop(0)
            at = rim_start(y_side, pos[1], fy, PAD)
            cut = []
            for f, width in enumerate(widths):
                start = rim_start(x_side, pos[0], fx, width)
                cut += [
                    ext[pl.ds(pl.multiple_of(f * rows + fy * (start + x) + at, 8), PAD), :]
                    for x in range(width)
                ]
            cut.append(jnp.zeros((PAD, LANES), F32))
            send[...] = jnp.concatenate(cut, 0).astype(BF16)


def solve_kernel(counts, *refs):
    it = iter(refs)
    pos, chip, ext, local_potential, refine, coarsen = (next(it) for _ in range(6))
    x_sides, y_sides = sides(counts[0]), sides(counts[1])
    xy_sides = [(a, b) for a in x_sides for b in y_sides]
    rho_x, rho_y, rho_xy = ([next(it) for _ in s] for s in (x_sides, y_sides, xy_sides))
    fld_x, fld_y, fld_xy = ([next(it) for _ in s] for s in (x_sides, y_sides, xy_sides))
    effective, potential, coarse, wide, fine, v0, v1, src, flat = it
    cx, cy, cz = pos[0], pos[1], pos[2]
    bx = chip.shape[0] // BY
    fx, fy = 2 * bx, 2 * BY
    ry, rc = fy + 2 * PAD, BY + 2 * PAD
    qx = fx + 2 * WV

    coarse[...] = jnp.zeros_like(coarse)
    for x in range(bx):
        coarse[WC + x, PAD : PAD + BY, :] = chip[x * BY : (x + 1) * BY, :]
    for side, ref in zip(x_sides, rho_x):
        at = halo_start(side, cx, 0, WC + bx)
        block = ref[...].astype(F32)
        for x in range(WC):
            coarse[at + x, PAD : PAD + BY, :] = block[x * BY : (x + 1) * BY, :]
    for side, ref in zip(y_sides, rho_y):
        at = pl.multiple_of(halo_start(side, cy, 0, PAD + BY), 8)
        block = ref[...].astype(F32)
        for x in range(bx):
            coarse[WC + x, pl.ds(at, PAD), :] = block[x * PAD : (x + 1) * PAD, :]
    for (x_side, y_side), ref in zip(xy_sides, rho_xy):
        at_x = halo_start(x_side, cx, 0, WC + bx)
        at = pl.multiple_of(halo_start(y_side, cy, 0, PAD + BY), 8)
        block = ref[...].astype(F32)
        for x in range(WC):
            coarse[at_x + x, pl.ds(at, PAD), :] = block[x * PAD : (x + 1) * PAD, :]

    v0[...] = jnp.zeros_like(v0)
    src[...] = jnp.zeros_like(src)
    for f, (ref, width) in enumerate(((v0, WV), (src, WS))):
        rows = f * fx * fy
        for x in range(fx):
            ref[WV + x, PAD : PAD + fy, :] = ext[rows + x * fy : rows + (x + 1) * fy, :]
        done = f * WV
        for side, got in zip(x_sides, fld_x):
            at = halo_start(side, cx, WV - width, WV + fx)
            for x in range(width):
                ref[at + x, PAD : PAD + fy, :] = got[(done + x) * fy : (done + x + 1) * fy, :].astype(F32)
        for side, got in zip(y_sides, fld_y):
            at = pl.multiple_of(halo_start(side, cy, 0, PAD + fy), 8)
            block = got[f * fx * PAD : (f + 1) * fx * PAD, :].astype(F32)
            for x in range(fx):
                ref[WV + x, pl.ds(at, PAD), :] = block[x * PAD : (x + 1) * PAD, :]
        for (x_side, y_side), got in zip(xy_sides, fld_xy):
            at_x = halo_start(x_side, cx, WV - width, WV + fx)
            at = pl.multiple_of(halo_start(y_side, cy, 0, PAD + fy), 8)
            block = got[...].astype(F32)
            for x in range(width):
                ref[at_x + x, pl.ds(at, PAD), :] = block[(done + x) * PAD : (done + x + 1) * PAD, :]

    cells = (bx + 2 * WC) * rc
    wide[...] = exact_dot(coarse[...].reshape(cells, LANES), refine[0])
    for p in range(bx + 2 * WC):
        base, half = p * rc + PAD // 2, ry // 2
        here = 0.75 * wide[pl.ds(base, half), :]
        fine[pl.ds(p * ry, half, stride=2), :] = here + 0.25 * wide[pl.ds(base - 1, half), :]
        fine[pl.ds(p * ry + 1, half, stride=2), :] = here + 0.25 * wide[pl.ds(base + 1, half), :]
    for q in range(1, qx - 1):
        at = q - WV
        here, other = at // 2 + WC, at // 2 + WC + (1 if at % 2 else -1)
        refined = 0.75 * fine[pl.ds(here * ry, ry), :] + 0.25 * fine[pl.ds(other * ry, ry), :]
        src[q] = math.pi * (refined - src[q])

    row = lax.broadcasted_iota(jnp.int32, (ry, LANES), 0) - PAD + fy * cy
    lane = lane_iota(ry) - ZOFF + 2 * BZ * cz
    inside = (row >= 0) & (row < fy * counts[1]) & (lane >= 0) & (lane < 2 * BZ * counts[2])
    share = jnp.where(inside, 1.0 / 6.0, 0.0)
    old, new = v0, v1
    for sweep in range(SWEEPS):
        for q in range(sweep + 1, qx - sweep - 1):
            at = q - WV + fx * cx
            here = old[q]
            total = old[q - 1] + old[q + 1]
            total = total + pltpu.roll(here, 1, 0) + pltpu.roll(here, ry - 1, 0)
            total = total + pltpu.roll(here, 1, 1) + pltpu.roll(here, LANES - 1, 1)
            total = (total + src[q]) * share
            if q < WV or q >= WV + fx:
                total = jnp.where((at >= 0) & (at < fx * counts[0]), total, 0.0)
            new[q] = total
        old, new = new, old

    groups = fy // 4
    lane = lane_iota(groups)
    for x in range(fx):
        r = [old[WV + x, pl.ds(PAD + k, groups, stride=4), :] for k in range(4)]
        r1, r2 = pltpu.roll(r[1], 80, 1), pltpu.roll(r[2], 48, 1)
        potential[pl.ds(3 * groups * x, groups, stride=3), :] = jnp.where(lane < 96, pltpu.roll(r[0], 112, 1), r1)
        potential[pl.ds(3 * groups * x + 1, groups, stride=3), :] = jnp.where(lane < 64, r1, r2)
        potential[pl.ds(3 * groups * x + 2, groups, stride=3), :] = jnp.where(lane < 32, r2, pltpu.roll(r[3], 16, 1))

    pieces = []
    for x in range(bx):
        q = WV + 2 * x
        fine[pl.ds(x * ry, ry), :] = 0.125 * (old[q - 1] + old[q + 2]) + 0.375 * (old[q] + old[q + 1])
        rows = [fine[pl.ds(x * ry + PAD + k, BY, stride=2), :] for k in (-1, 0, 1, 2)]
        pieces.append(0.125 * (rows[0] + rows[3]) + 0.375 * (rows[1] + rows[2]))
    back = exact_dot(jnp.concatenate(pieces, 0), coarsen[...])
    rho = (3.0 / math.pi) * pltpu.roll(chip[...], jnp.where(cz == 0, 0, LANES - BZ), 1)
    safe = jnp.where(rho > 0.0, rho, 1.0)
    root = jnp.exp(jnp.log(safe) * (1.0 / 3.0))
    root = root - (root - safe / (root * root)) * (1.0 / 3.0)
    flat[...] = back - jnp.where(rho > 0.0, root, 0.0)

    per = 384 // BZ
    groups = flat.shape[0] // per
    lane = lane_iota(groups)
    r = [pltpu.roll(flat[pl.ds(k, groups, stride=per), :], BZ * k % LANES, 1) for k in range(per)]
    for j in range(3):
        tile = None
        for k in range(per):
            low, high = BZ * k - LANES * j, BZ * (k + 1) - LANES * j
            if high > 0 and low < LANES:
                tile = r[k] if tile is None else jnp.where(lane >= low, r[k], tile)
        wide[pl.ds(j, groups, stride=3), :] = tile
    tiles = BY * BZ // LANES
    for t in range(tiles):
        cut = slice(t * LANES, (t + 1) * LANES)
        effective[:, cut] = wide[pl.ds(t, bx, stride=tiles), :] + local_potential[pl.ds(t, bx, stride=tiles), :]


def apply_kernel(counts, *refs):
    it = iter(refs)
    pos, orb, effective, zf, spread, masks = (next(it) for _ in range(6))
    x_sides, y_sides = sides(counts[0]), sides(counts[1])
    x_faces, y_faces = [next(it) for _ in x_sides], [next(it) for _ in y_sides]
    out, held, result, zbuf, load, face_load, store = it
    cx, cy = pos[0], pos[1]
    bx, bands, width = result.shape
    chunk = 16
    loads = [pltpu.make_async_copy(orb.at[x], held.at[x + 1], load.at[x]) for x in range(bx)]
    for copy in loads:
        copy.start()
    face_loads = []
    if x_sides == ("swap",):
        held[jnp.where(cx == 0, 0, bx + 1)] = jnp.zeros((bands, width), BF16)
    for i, (side, face) in enumerate(zip(x_sides, x_faces)):
        at = halo_start(side, cx, 0, bx + 1)
        face_loads.append(pltpu.make_async_copy(face, held.at[at], face_load.at[i]))
        face_loads[-1].start()
    for copy in loads + face_loads:
        copy.wait()
    low_mask, high_mask = masks[0:1, :], masks[1:2, :]
    lane = lane_iota(chunk)
    stores = []
    for x in range(bx):
        scale = effective[x : x + 1, :] + 3.0
        zbuf[...] = jnp.dot(zf[x], spread[0], preferred_element_type=F32)

        def body(i, carry, x=x, scale=scale):
            rows = pl.ds(pl.multiple_of(i * chunk, chunk), chunk)
            here = held[x + 1, rows, :].astype(F32)
            total = held[x, rows, :].astype(F32) + held[x + 2, rows, :].astype(F32) + zbuf[rows, :]
            total = total + pltpu.roll(here, 1, 1) * low_mask + pltpu.roll(here, width - 1, 1) * high_mask
            below, above = pltpu.roll(here, BZ, 1), pltpu.roll(here, width - BZ, 1)
            if y_sides == ("swap",):
                halo = pltpu.roll(y_faces[0][x, rows, :].astype(F32), jnp.where(cy == 0, LANES - BZ, BZ), 1)
                low, high = jnp.where(cy == 0, 0.0, halo), jnp.where(cy == 0, halo, 0.0)
            else:
                low = pltpu.roll(y_faces[0][x, rows, :].astype(F32), BZ, 1)
                high = pltpu.roll(y_faces[1][x, rows, :].astype(F32), LANES - BZ, 1)
            below = jnp.concatenate([jnp.where(lane < BZ, low, below[:, :LANES]), below[:, LANES:]], 1)
            above = jnp.concatenate([above[:, :-LANES], jnp.where(lane >= LANES - BZ, high, above[:, -LANES:])], 1)
            total = total + below + above
            result[x, rows, :] = (scale * here - 0.5 * total).astype(BF16)
            return carry

        lax.fori_loop(0, bands // chunk, body, 0)
        stores.append(pltpu.make_async_copy(result.at[x], out.at[x], store.at[x]))
        stores[-1].start()
    for copy in stores:
        copy.wait()


def vmem():
    return pl.BlockSpec(memory_space=pltpu.VMEM)


def smem():
    return pl.BlockSpec(memory_space=pltpu.SMEM)


def local(mesh, orbitals, occupations, previous, compensation, local_potential):
    domains, groups = mesh.shape["dom"], mesh.shape["band"]
    split_z = 2
    split_y = min(4, domains // 4)
    counts = (domains // (split_y * split_z), split_y, split_z)
    position = lax.axis_index("dom")
    cx, cy, cz = position // (split_y * split_z), position // split_z % split_y, position % split_z
    pos = jnp.stack([cx, cy, cz]).astype(jnp.int32)
    bands, _, bx, width = orbitals.shape
    tiles = width // LANES
    fx, fy = 2 * bx, 2 * BY
    x_sides, y_sides = sides(counts[0]), sides(counts[1])
    xy_sides = [(a, b) for a in x_sides for b in y_sides]
    params = pltpu.CompilerParams(vmem_limit_bytes=24 * 2**20)

    def shape(*dims, dtype=F32):
        return jax.ShapeDtypeStruct(dims, dtype)

    flat = [a.reshape(fx * fy * 2 * BZ // LANES, LANES) for a in (previous, compensation)]
    mate_fields = fetch(jnp.concatenate(flat, 0).astype(BF16), counts, {2: "swap"})

    orb = jnp.transpose(orbitals.reshape(bands, bx, width), (1, 0, 2))
    grid_spec = pltpu.PrefetchScalarGridSpec(
        num_scalar_prefetch=1,
        grid=(bx,),
        in_specs=[
            pl.BlockSpec((1, bands, width), lambda x, pos: (x, 0, 0)),
            pl.BlockSpec((bands, 1), lambda x, pos: (0, 0)),
            pl.BlockSpec((1, width, LANES), lambda x, pos: (pos[2], 0, 0)),
        ],
        out_specs=[
            pl.BlockSpec((bx * tiles, LANES), lambda x, pos: (0, 0)),
            pl.BlockSpec((1, bands, LANES), lambda x, pos: (x, 0, 0)),
        ]
        + [pl.BlockSpec((bands, width), lambda x, pos: (0, 0)) for _ in x_sides]
        + [pl.BlockSpec((1, bands, LANES), lambda x, pos: (x, 0, 0)) for _ in y_sides],
    )
    part, z_face, *faces = pl.pallas_call(
        functools.partial(density_kernel, counts),
        grid_spec=grid_spec,
        out_shape=[shape(bx * tiles, LANES), shape(bx, bands, LANES, dtype=BF16)]
        + [shape(bands, width, dtype=BF16) for _ in x_sides]
        + [shape(bx, bands, LANES, dtype=BF16) for _ in y_sides],
        compiler_params=params,
        name="density",
    )(pos, orb, occupations.reshape(bands, 1), jnp.asarray(z_pick(), BF16))
    x_faces = [fetch(f, counts, {0: s}) for s, f in zip(x_sides, faces)]
    parts = [part]
    for step in range(1, groups):
        route = [(i, (i + step) % groups) for i in range(groups)]
        parts.append(lax.ppermute(part, "band", route))
    z_face = fetch(z_face, counts, {2: "swap"})
    y_faces = [fetch(f, counts, {1: s}) for s, f in zip(y_sides, faces[len(x_sides) :])]

    rim_rows = [(WV + WS) * fy] * len(x_sides) + [2 * fx * PAD] * len(y_sides)
    rim_rows += [(WV + WS + 1) * PAD] * len(xy_sides)
    ext, *rims = pl.pallas_call(
        functools.partial(field_kernel, counts),
        in_specs=[smem(), vmem(), vmem(), vmem()],
        out_specs=[vmem()] * (1 + len(rim_rows)),
        out_shape=[shape(2 * fx * fy, LANES)] + [shape(n, LANES, dtype=BF16) for n in rim_rows],
        scratch_shapes=[pltpu.VMEM((2 * flat[0].shape[0], LANES), F32)],
        compiler_params=params,
        name="fields",
    )(pos, *flat, mate_fields)
    moves = [{0: s} for s in x_sides] + [{1: s} for s in y_sides] + [{0: a, 1: b} for a, b in xy_sides]
    fields = [fetch(r, counts, m) for r, m in zip(rims, moves)]

    rho = pl.pallas_call(
        functools.partial(total_kernel, 1.0 / (bands * groups)),
        in_specs=[smem()] + [vmem()] * groups,
        out_specs=vmem(),
        out_shape=shape(bx * BY, LANES),
        scratch_shapes=[pltpu.VMEM((bx * tiles, LANES), F32)],
        compiler_params=params,
        name="total",
    )(pos, *parts)
    chip = rho + fetch(rho, counts, {2: "swap"})
    cells = chip.reshape(bx, BY, LANES)
    densities = []
    for move in moves:
        cut = cells
        if 0 in move:
            cut = lax.dynamic_slice_in_dim(cut, rim_start(move[0], cx, bx, WC), WC, 0)
        if 1 in move:
            cut = lax.dynamic_slice_in_dim(cut, rim_start(move[1], cy, BY, PAD), PAD, 1)
        cut = cut.astype(BF16).reshape(-1, LANES)
        densities.append(fetch(cut, counts, move))

    rc, ry, qx = BY + 2 * PAD, fy + 2 * PAD, fx + 2 * WV
    n_moves = len(moves)
    effective, potential = pl.pallas_call(
        functools.partial(solve_kernel, counts),
        grid_spec=pltpu.PrefetchScalarGridSpec(
            num_scalar_prefetch=1,
            grid=(1,),
            in_specs=[pl.BlockSpec(a, lambda i, pos, n=len(a): (0,) * n) for a in (chip.shape, ext.shape)]
            + [pl.BlockSpec((bx * tiles, LANES), lambda i, pos: (0, 0))]
            + [pl.BlockSpec((1, LANES, LANES), lambda i, pos: (pos[2], 0, 0))]
            + [pl.BlockSpec((LANES, LANES), lambda i, pos: (0, 0))]
            + [pl.BlockSpec(a.shape, lambda i, pos: (0, 0)) for a in densities + fields],
            out_specs=[
                pl.BlockSpec((bx, width), lambda i, pos: (0, 0)),
                pl.BlockSpec(flat[0].shape, lambda i, pos: (0, 0)),
            ],
            scratch_shapes=[
                pltpu.VMEM((bx + 2 * WC, rc, LANES), F32),
                pltpu.VMEM(((bx + 2 * WC) * rc, LANES), F32),
                pltpu.VMEM(((bx + 2 * WC) * ry, LANES), F32),
                pltpu.VMEM((qx, ry, LANES), F32),
                pltpu.VMEM((qx, ry, LANES), F32),
                pltpu.VMEM((qx, ry, LANES), F32),
                pltpu.VMEM((bx * BY, LANES), F32),
            ],
        ),
        out_shape=[shape(bx, width), shape(*flat[0].shape)],
        compiler_params=params,
        name="solve",
    )(
        pos,
        chip,
        ext,
        local_potential.reshape(bx * tiles, LANES),
        jnp.asarray(z_refine(), BF16),
        jnp.asarray(z_coarsen(), BF16),
        *densities,
        *fields,
    )

    hbm = pl.BlockSpec(memory_space=pl.ANY)
    applied = pl.pallas_call(
        functools.partial(apply_kernel, counts),
        grid_spec=pltpu.PrefetchScalarGridSpec(
            num_scalar_prefetch=1,
            grid=(1,),
            in_specs=[
                hbm,
                pl.BlockSpec((bx, width), lambda i, pos: (0, 0)),
                pl.BlockSpec(z_face.shape, lambda i, pos: (0, 0, 0)),
                pl.BlockSpec((1, LANES, width), lambda i, pos: (pos[2], 0, 0)),
                pl.BlockSpec((8, width), lambda i, pos: (0, 0)),
            ]
            + [hbm for _ in x_faces]
            + [pl.BlockSpec(a.shape, lambda i, pos: (0, 0, 0)) for a in y_faces],
            out_specs=hbm,
            scratch_shapes=[
                pltpu.VMEM((bx + 2, bands, width), BF16),
                pltpu.VMEM((bx, bands, width), BF16),
                pltpu.VMEM((bands, width), F32),
                pltpu.SemaphoreType.DMA((bx,)),
                pltpu.SemaphoreType.DMA((2,)),
                pltpu.SemaphoreType.DMA((bx,)),
            ],
        ),
        out_shape=shape(bx, bands, width, dtype=BF16),
        compiler_params=params,
        name="apply",
    )(pos, orb, effective, z_face, jnp.asarray(z_spread(), BF16), jnp.asarray(z_masks()), *x_faces, *y_faces)
    applied = jnp.transpose(applied, (1, 0, 2)).reshape(orbitals.shape)
    return applied, potential.reshape(previous.shape)


def solution(mesh):
    return jax.shard_map(
        functools.partial(local, mesh),
        mesh=mesh,
        in_specs=(
            P("band", "dom", None, None),
            P("band"),
            P("dom", None, None),
            P("dom", None, None),
            P("dom", None, None),
        ),
        out_specs=(P("band", "dom", None, None), P("dom", None, None)),
        check_vma=False,
    )
```

```python
import functools
import math

import jax
import jax.numpy as jnp
import numpy as np
from jax import lax
from jax.experimental import pallas as pl
from jax.experimental.pallas import tpu as pltpu
from jax.sharding import PartitionSpec as P

BY = 24
BZ = 48
SWEEPS = 4

F32, BF16 = jnp.float32, jnp.bfloat16
LANES = 128
PAD = 8
ZOFF = 16
WV = SWEEPS + 1
WS = SWEEPS
WC = WS // 2 + 1


def sides(count):
    return ("swap",) if count == 2 else ("lo", "hi")


def fetch(block, counts, moves):
    pairs = []
    for target in np.ndindex(*counts):
        source = list(target)
        for axis, side in moves.items():
            source[axis] = {"swap": 1 - target[axis], "lo": target[axis] - 1, "hi": target[axis] + 1}[side]
        if all(0 <= s < n for s, n in zip(source, counts)):
            pairs.append((int(np.ravel_multi_index(source, counts)), int(np.ravel_multi_index(target, counts))))
    return lax.ppermute(block, "dom", pairs)


def rim_start(side, coord, length, width):
    if side == "swap":
        return jnp.where(coord == 0, length - width, 0)
    return length - width if side == "lo" else 0


def halo_start(side, coord, low, high):
    if side == "swap":
        return jnp.where(coord == 0, high, low)
    return low if side == "lo" else high


def lane_iota(rows):
    return lax.broadcasted_iota(jnp.int32, (rows, LANES), 1)


def exact_dot(value, weights):
    high = value.astype(BF16)
    rest = value - high.astype(F32)
    middle = rest.astype(BF16)
    low = (rest - middle.astype(F32)).astype(BF16)
    dot = functools.partial(jnp.dot, preferred_element_type=F32)
    return dot(high, weights) + (dot(middle, weights) + dot(low, weights))


def grid2(rows, columns):
    shape = (rows, columns)
    return (lax.broadcasted_iota(jnp.int32, shape, d) for d in (0, 1))


def z_refine(core):
    cell, lane = grid2(LANES, LANES)
    fine = lane - ZOFF + 2 * BZ * core
    here = fine >> 1
    other = here + 2 * (fine & 1) - 1
    return jnp.where(cell == here, 0.75, jnp.where(cell == other, 0.25, 0.0)).astype(BF16)


def z_coarsen():
    lane, cell = grid2(LANES, LANES)
    step = lane - ZOFF - 2 * cell
    w = jnp.where((step == 0) | (step == 1), 0.375, jnp.where((step == -1) | (step == 2), 0.125, 0.0))
    return jnp.where(cell < BZ, w, 0.0).astype(BF16)


def z_pick(core):
    lane, y = grid2(BY * BZ, LANES)
    return jnp.where(lane == BZ * y + jnp.where(core == 0, BZ - 1, 0), 1.0, 0.0).astype(BF16)


def z_spread(core):
    y, lane = grid2(LANES, BY * BZ)
    return jnp.where(lane == BZ * y + jnp.where(core == 0, BZ - 1, 0), -0.5, 0.0).astype(BF16)


def stencil(first, columns):
    source, lane = grid2(4 * LANES, columns)
    step = source - LANES - lane
    z = (lax.broadcasted_iota(jnp.int32, (1, columns), 1) + first) % BZ
    up = jnp.where(z == BZ - 1, 2 * BY * BZ, 1)
    down = jnp.where(z == 0, 2 * BY * BZ, -1)
    near = (step == up) | (step == down) | (step == BZ) | (step == -BZ)
    return jnp.where(near, -0.5, jnp.where(step == 0, 3.0, 0.0)).astype(BF16)


def density_kernel(counts, pos, orb, occ, part, zf, *refs):
    faces, (held, load) = refs[:-2], refs[-2:]
    planes, bands, width = held.shape
    tiles = width // LANES
    x_sides, y_sides = sides(counts[0]), sides(counts[1])
    x_faces, y_faces = faces[: len(x_sides)], faces[len(x_sides) :]
    loads = [pltpu.make_async_copy(orb.at[x], held.at[x], load.at[x]) for x in range(planes)]
    for copy in loads:
        copy.start()
    rows = jnp.broadcast_to(occ[...], (LANES, occ.shape[1]))
    weight = [rows[:, b : b + LANES].T for b in range(0, occ.shape[1], LANES)]
    weight = jnp.concatenate(weight, 0)[:bands]
    pick = z_pick(pos[2])
    for x in range(planes):
        loads[x].wait()
        for t in range(tiles):
            f = held[x, :, t * LANES : (t + 1) * LANES].astype(F32)
            part[tiles * x + t : tiles * x + t + 1, :] = jnp.sum(f * f * weight, axis=0, keepdims=True)
        zf[x] = jnp.dot(held[x], pick, preferred_element_type=F32).astype(BF16)
        for side, face in zip(y_sides, y_faces):
            start = rim_start(side, pos[1], width, LANES)
            face[x] = held[x, :, pl.ds(pl.multiple_of(start, LANES), LANES)]
    for side, face in zip(x_sides, x_faces):
        face[...] = held[rim_start(side, pos[0], planes, 1)]


def total_kernel(scale, pos, *refs):
    parts, out, flat = refs[:-2], refs[-2], refs[-1]
    total = parts[0][...]
    for part in parts[1:]:
        total = total + part[...]
    flat[...] = total * scale
    per = 384 // BZ
    groups = flat.shape[0] // 3
    lane = lane_iota(groups)
    shift = jnp.where(pos[2] == 0, 0, BZ)
    tile = [flat[pl.ds(j, groups, stride=3), :] for j in range(3)]
    for k in range(per):
        at, off = divmod(BZ * k, LANES)
        row = pltpu.roll(tile[at], (LANES - off) % LANES, 1) if off else tile[at]
        if off + BZ > LANES:
            row = jnp.where(lane < LANES - off, row, pltpu.roll(tile[at + 1], LANES - off, 1))
        row = jnp.where(lane < BZ, row, 0.0)
        out[pl.ds(k, groups, stride=per), :] = pltpu.roll(row, shift, 1)


def field_rows(ref, groups):
    lane = lane_iota(groups)
    a, b, c = (ref[pl.ds(j, groups, stride=3), :] for j in range(3))
    return (
        pltpu.roll(a, 16, 1),
        jnp.where(lane < 48, pltpu.roll(a, 48, 1), pltpu.roll(b, 48, 1)),
        jnp.where(lane < 80, pltpu.roll(b, 80, 1), pltpu.roll(c, 80, 1)),
        pltpu.roll(c, 112, 1),
    )


def field_kernel(counts, pos, prev, comp, mate_prev, mate_comp, ext, *refs):
    sends = list(refs)
    fx, fy = prev.shape[0] * LANES // (2 * BY * 2 * BZ), 2 * BY
    groups = prev.shape[0] // 3
    lane = lane_iota(groups)
    own = (lane >= ZOFF) & (lane < ZOFF + 2 * BZ)
    first = pos[2] == 0
    shift = jnp.where(first, 2 * BZ, LANES - 2 * BZ)
    edge_low = jnp.where(first, ZOFF + 2 * BZ, 0)
    edge_high = jnp.where(first, LANES, ZOFF)
    edge = (lane >= edge_low) & (lane < edge_high)
    rows = fx * fy
    for f, (ref, mate) in enumerate(((prev, mate_prev), (comp, mate_comp))):
        mine = field_rows(ref, groups)
        theirs = field_rows(mate, groups)
        for k in range(4):
            halo = jnp.where(edge, pltpu.roll(theirs[k], shift, 1), 0.0)
            ext[pl.ds(f * rows + k, groups, stride=4), :] = jnp.where(own, mine[k], halo)
    widths = (WV, WS)
    x_sides, y_sides = sides(counts[0]), sides(counts[1])
    for side in x_sides:
        send, done = sends.pop(0), 0
        for f, width in enumerate(widths):
            start = f * rows + fy * rim_start(side, pos[0], fx, width)
            send[pl.ds(done, width * fy), :] = ext[pl.ds(pl.multiple_of(start, 8), width * fy), :].astype(BF16)
            done += width * fy
    for side in y_sides:
        send = sends.pop(0)
        at = rim_start(side, pos[1], fy, PAD)
        for f in range(2):
            cut = [ext[pl.ds(pl.multiple_of(f * rows + fy * x + at, 8), PAD), :] for x in range(fx)]
            send[pl.ds(f * fx * PAD, fx * PAD), :] = jnp.concatenate(cut, 0).astype(BF16)
    for x_side in x_sides:
        for y_side in y_sides:
            send = sends.pop(0)
            at = rim_start(y_side, pos[1], fy, PAD)
            cut = []
            for f, width in enumerate(widths):
                start = rim_start(x_side, pos[0], fx, width)
                cut += [
                    ext[pl.ds(pl.multiple_of(f * rows + fy * (start + x) + at, 8), PAD), :]
                    for x in range(width)
                ]
            cut.append(jnp.zeros((PAD, LANES), F32))
            send[...] = jnp.concatenate(cut, 0).astype(BF16)


def solve_kernel(counts, *refs):
    it = iter(refs)
    pos, chip, ext, local_potential = (next(it) for _ in range(4))
    x_sides, y_sides = sides(counts[0]), sides(counts[1])
    xy_sides = [(a, b) for a in x_sides for b in y_sides]
    rho_x, rho_y, rho_xy = ([next(it) for _ in s] for s in (x_sides, y_sides, xy_sides))
    fld_x, fld_y, fld_xy = ([next(it) for _ in s] for s in (x_sides, y_sides, xy_sides))
    effective, potential, coarse, wide, fine, v0, v1, src, flat = it
    cx, cy, cz = pos[0], pos[1], pos[2]
    bx = chip.shape[0] // BY
    fx, fy = 2 * bx, 2 * BY
    ry, rc = fy + 2 * PAD, BY + 2 * PAD
    qx = fx + 2 * WV

    coarse[...] = jnp.zeros_like(coarse)
    for x in range(bx):
        coarse[WC + x, PAD : PAD + BY, :] = chip[x * BY : (x + 1) * BY, :]
    for side, ref in zip(x_sides, rho_x):
        at = halo_start(side, cx, 0, WC + bx)
        block = ref[...].astype(F32)
        for x in range(WC):
            coarse[at + x, PAD : PAD + BY, :] = block[x * BY : (x + 1) * BY, :]
    for side, ref in zip(y_sides, rho_y):
        at = pl.multiple_of(halo_start(side, cy, 0, PAD + BY), 8)
        block = ref[...].astype(F32)
        for x in range(bx):
            coarse[WC + x, pl.ds(at, PAD), :] = block[x * PAD : (x + 1) * PAD, :]
    for (x_side, y_side), ref in zip(xy_sides, rho_xy):
        at_x = halo_start(x_side, cx, 0, WC + bx)
        at = pl.multiple_of(halo_start(y_side, cy, 0, PAD + BY), 8)
        block = ref[...].astype(F32)
        for x in range(WC):
            coarse[at_x + x, pl.ds(at, PAD), :] = block[x * PAD : (x + 1) * PAD, :]

    v0[...] = jnp.zeros_like(v0)
    src[...] = jnp.zeros_like(src)
    for f, (ref, width) in enumerate(((v0, WV), (src, WS))):
        rows = f * fx * fy
        for x in range(fx):
            ref[WV + x, PAD : PAD + fy, :] = ext[rows + x * fy : rows + (x + 1) * fy, :]
        done = f * WV
        for side, got in zip(x_sides, fld_x):
            at = halo_start(side, cx, WV - width, WV + fx)
            for x in range(width):
                ref[at + x, PAD : PAD + fy, :] = got[(done + x) * fy : (done + x + 1) * fy, :].astype(F32)
        for side, got in zip(y_sides, fld_y):
            at = pl.multiple_of(halo_start(side, cy, 0, PAD + fy), 8)
            block = got[f * fx * PAD : (f + 1) * fx * PAD, :].astype(F32)
            for x in range(fx):
                ref[WV + x, pl.ds(at, PAD), :] = block[x * PAD : (x + 1) * PAD, :]
        for (x_side, y_side), got in zip(xy_sides, fld_xy):
            at_x = halo_start(x_side, cx, WV - width, WV + fx)
            at = pl.multiple_of(halo_start(y_side, cy, 0, PAD + fy), 8)
            block = got[...].astype(F32)
            for x in range(width):
                ref[at_x + x, pl.ds(at, PAD), :] = block[(done + x) * PAD : (done + x + 1) * PAD, :]

    cells = (bx + 2 * WC) * rc
    wide[...] = exact_dot(coarse[...].reshape(cells, LANES), z_refine(cz))
    for p in range(bx + 2 * WC):
        base, half = p * rc + PAD // 2, ry // 2
        here = 0.75 * wide[pl.ds(base, half), :]
        fine[pl.ds(p * ry, half, stride=2), :] = here + 0.25 * wide[pl.ds(base - 1, half), :]
        fine[pl.ds(p * ry + 1, half, stride=2), :] = here + 0.25 * wide[pl.ds(base + 1, half), :]
    for q in range(1, qx - 1):
        at = q - WV
        here, other = at // 2 + WC, at // 2 + WC + (1 if at % 2 else -1)
        refined = 0.75 * fine[pl.ds(here * ry, ry), :] + 0.25 * fine[pl.ds(other * ry, ry), :]
        src[q] = math.pi * (refined - src[q])

    row = lax.broadcasted_iota(jnp.int32, (ry, LANES), 0) - PAD + fy * cy
    lane = lane_iota(ry) - ZOFF + 2 * BZ * cz
    inside = (row >= 0) & (row < fy * counts[1]) & (lane >= 0) & (lane < 2 * BZ * counts[2])
    share = jnp.where(inside, 1.0 / 6.0, 0.0)
    old, new = v0, v1
    for sweep in range(SWEEPS):
        for q in range(sweep + 1, qx - sweep - 1):
            at = q - WV + fx * cx
            here = old[q]
            total = old[q - 1] + old[q + 1]
            total = total + pltpu.roll(here, 1, 0) + pltpu.roll(here, ry - 1, 0)
            total = total + pltpu.roll(here, 1, 1) + pltpu.roll(here, LANES - 1, 1)
            total = (total + src[q]) * share
            if q < WV or q >= WV + fx:
                total = jnp.where((at >= 0) & (at < fx * counts[0]), total, 0.0)
            new[q] = total
        old, new = new, old

    groups = fy // 4
    lane = lane_iota(groups)
    for x in range(fx):
        r = [old[WV + x, pl.ds(PAD + k, groups, stride=4), :] for k in range(4)]
        r1, r2 = pltpu.roll(r[1], 80, 1), pltpu.roll(r[2], 48, 1)
        potential[pl.ds(3 * groups * x, groups, stride=3), :] = jnp.where(lane < 96, pltpu.roll(r[0], 112, 1), r1)
        potential[pl.ds(3 * groups * x + 1, groups, stride=3), :] = jnp.where(lane < 64, r1, r2)
        potential[pl.ds(3 * groups * x + 2, groups, stride=3), :] = jnp.where(lane < 32, r2, pltpu.roll(r[3], 16, 1))

    pieces = []
    for x in range(bx):
        q = WV + 2 * x
        fine[pl.ds(x * ry, ry), :] = 0.125 * (old[q - 1] + old[q + 2]) + 0.375 * (old[q] + old[q + 1])
        rows = [fine[pl.ds(x * ry + PAD + k, BY, stride=2), :] for k in (-1, 0, 1, 2)]
        pieces.append(0.125 * (rows[0] + rows[3]) + 0.375 * (rows[1] + rows[2]))
    back = exact_dot(jnp.concatenate(pieces, 0), z_coarsen())
    rho = (3.0 / math.pi) * pltpu.roll(chip[...], jnp.where(cz == 0, 0, LANES - BZ), 1)
    safe = jnp.where(rho > 0.0, rho, 1.0)
    root = jnp.exp(jnp.log(safe) * (1.0 / 3.0))
    root = root - (root - safe / (root * root)) * (1.0 / 3.0)
    flat[...] = back - jnp.where(rho > 0.0, root, 0.0)

    per = 384 // BZ
    groups = flat.shape[0] // per
    lane = lane_iota(groups)
    r = [pltpu.roll(flat[pl.ds(k, groups, stride=per), :], BZ * k % LANES, 1) for k in range(per)]
    for j in range(3):
        tile = None
        for k in range(per):
            low, high = BZ * k - LANES * j, BZ * (k + 1) - LANES * j
            if high > 0 and low < LANES:
                tile = r[k] if tile is None else jnp.where(lane >= low, r[k], tile)
        wide[pl.ds(j, groups, stride=3), :] = tile
    tiles = BY * BZ // LANES
    for t in range(tiles):
        cut = slice(t * LANES, (t + 1) * LANES)
        effective[:, cut] = wide[pl.ds(t, bx, stride=tiles), :]
    for x in range(bx):
        effective[x : x + 1, :] = effective[x : x + 1, :] + local_potential[x]


def laplace_kernel(orb, out, held, load):
    planes, bands, width = held.shape
    copy = pltpu.make_async_copy(orb, held, load)
    copy.start()
    step = 2 * LANES
    weights = [stencil(step * p % BZ, step) for p in range(3)]
    copy.wait()
    for j in range(0, width, step):
        columns = min(step, width - j)
        first, last = max(j - LANES, 0), min(j + step + LANES, width)
        skip = first - (j - LANES)
        w = weights[j // step % 3][skip : skip + last - first, :columns]
        here = held[:, :, first:last].reshape(planes * bands, last - first)
        total = jnp.dot(here, w, preferred_element_type=F32).reshape(planes, bands, columns)
        for x in range(planes):
            near = [held[n, :, j : j + columns].astype(F32) for n in (x - 1, x + 1) if 0 <= n < planes]
            out[x, :, j : j + columns] = total[x] - 0.5 * sum(near)


def apply_kernel(counts, *refs):
    it = iter(refs)
    pos, orb, inner, effective, zf = (next(it) for _ in range(5))
    x_sides, y_sides = sides(counts[0]), sides(counts[1])
    x_faces, y_faces = [next(it) for _ in x_sides], [next(it) for _ in y_sides]
    out, held, result, load, store = it
    cx, cy = pos[0], pos[1]
    bx, bands, width = result.shape
    loads = [pltpu.make_async_copy(orb.at[x], held.at[x], load.at[x]) for x in range(bx)]
    for copy in loads:
        copy.start()
    spread = z_spread(pos[2])
    lane = lane_iota(bands)
    stores = []
    for x in range(bx):
        loads[x].wait()
        outer = jnp.dot(zf[x], spread, preferred_element_type=F32)
        low = high = None
        for side, face in zip(y_sides, y_faces):
            if side == "swap":
                halo = -0.5 * pltpu.roll(face[x].astype(F32), jnp.where(cy == 0, LANES - BZ, BZ), 1)
                low = jnp.where((lane < BZ) & (cy > 0), halo, 0.0)
                high = jnp.where((lane >= LANES - BZ) & (cy == 0), halo, 0.0)
            elif side == "lo":
                low = jnp.where(lane < BZ, -0.5 * pltpu.roll(face[x].astype(F32), BZ, 1), 0.0)
            else:
                high = jnp.where(lane >= LANES - BZ, -0.5 * pltpu.roll(face[x].astype(F32), LANES - BZ, 1), 0.0)
        for t in range(width // LANES):
            cut = slice(t * LANES, (t + 1) * LANES)
            total = inner[x, :, cut] + outer[:, cut] + effective[x : x + 1, cut] * held[x, :, cut].astype(F32)
            if t == 0:
                total = total + low
            if t == width // LANES - 1:
                total = total + high
            for side, face in zip(x_sides, x_faces):
                if x == 0 and side != "hi":
                    scale = jnp.where(cx > 0, -0.5, 0.0)
                    total = total + scale * face[:, cut].astype(F32)
                if x == bx - 1 and side != "lo":
                    scale = jnp.where(cx < counts[0] - 1, -0.5, 0.0)
                    total = total + scale * face[:, cut].astype(F32)
            result[x, :, cut] = total.astype(BF16)
        stores.append(pltpu.make_async_copy(result.at[x], out.at[x], store.at[x]))
        stores[-1].start()
    for copy in stores:
        copy.wait()


def vmem():
    return pl.BlockSpec(memory_space=pltpu.VMEM)


def smem():
    return pl.BlockSpec(memory_space=pltpu.SMEM)


def local(mesh, orbitals, occupations, previous, compensation, local_potential):
    domains, groups = mesh.shape["dom"], mesh.shape["band"]
    split_z = 2
    split_y = min(4, domains // 4)
    counts = (domains // (split_y * split_z), split_y, split_z)
    position = lax.axis_index("dom")
    cx, cy, cz = position // (split_y * split_z), position // split_z % split_y, position % split_z
    pos = jnp.stack([cx, cy, cz]).astype(jnp.int32)
    bands, _, bx, width = orbitals.shape
    tiles = width // LANES
    fx, fy = 2 * bx, 2 * BY
    x_sides, y_sides = sides(counts[0]), sides(counts[1])
    xy_sides = [(a, b) for a in x_sides for b in y_sides]

    def params(mib):
        return pltpu.CompilerParams(vmem_limit_bytes=mib * 2**20)

    def shape(*dims, dtype=F32):
        return jax.ShapeDtypeStruct(dims, dtype)

    flat = [a.reshape(fx * fy * 2 * BZ // LANES, LANES) for a in (previous, compensation)]
    mates = [fetch(a, counts, {2: "swap"}) for a in flat]

    hbm = pl.BlockSpec(memory_space=pltpu.HBM)
    orb = jnp.transpose(orbitals.reshape(bands, bx, width), (1, 0, 2))
    occupied = jnp.pad(occupations.reshape(1, bands), ((0, 0), (0, -bands % LANES)))
    part, z_face, *faces = pl.pallas_call(
        functools.partial(density_kernel, counts),
        in_specs=[smem(), hbm, vmem()],
        out_specs=[vmem()] * (2 + len(x_sides) + len(y_sides)),
        out_shape=[shape(bx * tiles, LANES), shape(bx, bands, LANES, dtype=BF16)]
        + [shape(bands, width, dtype=BF16) for _ in x_sides]
        + [shape(bx, bands, LANES, dtype=BF16) for _ in y_sides],
        scratch_shapes=[pltpu.VMEM((bx, bands, width), BF16), pltpu.SemaphoreType.DMA((bx,))],
        compiler_params=params(12),
        name="density",
    )(pos, orb, occupied)
    x_faces = [fetch(f, counts, {0: s}) for s, f in zip(x_sides, faces)]
    parts = [part]
    for step in range(1, groups):
        route = [(i, (i + step) % groups) for i in range(groups)]
        parts.append(lax.ppermute(part, "band", route))
    z_face = fetch(z_face, counts, {2: "swap"})
    y_faces = [fetch(f, counts, {1: s}) for s, f in zip(y_sides, faces[len(x_sides) :])]

    inner = pl.pallas_call(
        laplace_kernel,
        in_specs=[hbm],
        out_specs=vmem(),
        out_shape=shape(bx, bands, width),
        scratch_shapes=[pltpu.VMEM((bx, bands, width), BF16), pltpu.SemaphoreType.DMA(())],
        compiler_params=params(20),
        cost_estimate=pl.CostEstimate(flops=6 * 10**9, bytes_accessed=8 * 10**6, transcendentals=0),
        name="laplace",
    )(orb)

    rim_rows = [(WV + WS) * fy] * len(x_sides) + [2 * fx * PAD] * len(y_sides)
    rim_rows += [(WV + WS + 1) * PAD] * len(xy_sides)
    ext, *rims = pl.pallas_call(
        functools.partial(field_kernel, counts),
        in_specs=[smem()] + [vmem()] * 4,
        out_specs=[vmem()] * (1 + len(rim_rows)),
        out_shape=[shape(2 * fx * fy, LANES)] + [shape(n, LANES, dtype=BF16) for n in rim_rows],
        compiler_params=params(6),
        name="fields",
    )(pos, *flat, *mates)
    moves = [{0: s} for s in x_sides] + [{1: s} for s in y_sides] + [{0: a, 1: b} for a, b in xy_sides]
    fields = [fetch(r, counts, m) for r, m in zip(rims, moves)]

    rho = pl.pallas_call(
        functools.partial(total_kernel, 1.0 / (bands * groups)),
        in_specs=[smem()] + [vmem()] * groups,
        out_specs=vmem(),
        out_shape=shape(bx * BY, LANES),
        scratch_shapes=[pltpu.VMEM((bx * tiles, LANES), F32)],
        compiler_params=params(2),
        name="total",
    )(pos, *parts)
    chip = rho + fetch(rho, counts, {2: "swap"})
    cells = chip.reshape(bx, BY, LANES)
    densities = []
    for move in moves:
        cut = cells
        if 0 in move:
            cut = lax.dynamic_slice_in_dim(cut, rim_start(move[0], cx, bx, WC), WC, 0)
        if 1 in move:
            cut = lax.dynamic_slice_in_dim(cut, rim_start(move[1], cy, BY, PAD), PAD, 1)
        cut = cut.astype(BF16).reshape(-1, LANES)
        densities.append(fetch(cut, counts, move))

    rc, ry, qx = BY + 2 * PAD, fy + 2 * PAD, fx + 2 * WV
    local_rows = jnp.transpose(local_potential, (1, 0, 2))
    effective, potential = pl.pallas_call(
        functools.partial(solve_kernel, counts),
        in_specs=[smem()] + [vmem()] * (3 + len(densities) + len(fields)),
        out_specs=[vmem(), vmem()],
        scratch_shapes=[
            pltpu.VMEM((bx + 2 * WC, rc, LANES), F32),
            pltpu.VMEM(((bx + 2 * WC) * rc, LANES), F32),
            pltpu.VMEM(((bx + 2 * WC) * ry, LANES), F32),
            pltpu.VMEM((qx, ry, LANES), F32),
            pltpu.VMEM((qx, ry, LANES), F32),
            pltpu.VMEM((qx, ry, LANES), F32),
            pltpu.VMEM((bx * BY, LANES), F32),
        ],
        out_shape=[shape(bx, width), shape(*flat[0].shape)],
        compiler_params=params(10),
        name="solve",
    )(pos, chip, ext, local_rows, *densities, *fields)

    applied = pl.pallas_call(
        functools.partial(apply_kernel, counts),
        in_specs=[smem(), hbm] + [vmem()] * (3 + len(x_faces) + len(y_faces)),
        out_specs=hbm,
        scratch_shapes=[
            pltpu.VMEM((bx, bands, width), BF16),
            pltpu.VMEM((bx, bands, width), BF16),
            pltpu.SemaphoreType.DMA((bx,)),
            pltpu.SemaphoreType.DMA((bx,)),
        ],
        out_shape=shape(bx, bands, width, dtype=BF16),
        compiler_params=params(20),
        name="apply",
    )(pos, orb, inner, effective, z_face, *x_faces, *y_faces)
    applied = jnp.transpose(applied, (1, 0, 2)).reshape(orbitals.shape)
    return applied, potential.reshape(previous.shape)


def solution(mesh):
    return jax.shard_map(
        functools.partial(local, mesh),
        mesh=mesh,
        in_specs=(
            P("band", "dom", None, None),
            P("band"),
            P("dom", None, None),
            P("dom", None, None),
            P("dom", None, None),
        ),
        out_specs=(P("band", "dom", None, None), P("dom", None, None)),
        check_vma=False,
    )
```

```python
import functools
import math

import jax
import jax.numpy as jnp
import numpy as np
from jax import lax
from jax.experimental import pallas as pl
from jax.experimental.pallas import tpu as pltpu
from jax.sharding import PartitionSpec as P


BY = 24
BZ = 48
SWEEPS = 4

F32, BF16 = jnp.float32, jnp.bfloat16
LANES = 128
PAD = 8
ZOFF = 16
WV = SWEEPS + 1
WS = SWEEPS
WC = WS // 2 + 1


def sides(count):
    return ("swap",) if count == 2 else ("lo", "hi")


def fetch(block, counts, moves):
    pairs = []
    for target in np.ndindex(*counts):
        source = list(target)
        for axis, side in moves.items():
            source[axis] = {"swap": 1 - target[axis], "lo": target[axis] - 1, "hi": target[axis] + 1}[side]
        if all(0 <= s < n for s, n in zip(source, counts)):
            pairs.append((int(np.ravel_multi_index(source, counts)), int(np.ravel_multi_index(target, counts))))
    return lax.ppermute(block, "dom", pairs)


def rim_start(side, coord, length, width):
    if side == "swap":
        return jnp.where(coord == 0, length - width, 0)
    return length - width if side == "lo" else 0


def halo_start(side, coord, low, high):
    if side == "swap":
        return jnp.where(coord == 0, high, low)
    return low if side == "lo" else high


def position(counts):
    at = lax.axis_index("dom")
    return at // (counts[1] * counts[2]), at // counts[2] % counts[1], at % counts[2]


def lane_iota(rows):
    return lax.broadcasted_iota(jnp.int32, (rows, LANES), 1)


def exact_dot(value, weights):
    high = value.astype(BF16)
    rest = value - high.astype(F32)
    middle = rest.astype(BF16)
    low = (rest - middle.astype(F32)).astype(BF16)
    dot = functools.partial(jnp.dot, preferred_element_type=F32)
    return dot(high, weights) + (dot(middle, weights) + dot(low, weights))


def grid2(rows, columns):
    shape = (rows, columns)
    return (lax.broadcasted_iota(jnp.int32, shape, d) for d in (0, 1))


def z_refine(core):
    cell, lane = grid2(LANES, LANES)
    fine = lane - ZOFF + 2 * BZ * core
    here = fine >> 1
    other = here + 2 * (fine & 1) - 1
    return jnp.where(cell == here, 0.75, jnp.where(cell == other, 0.25, 0.0)).astype(BF16)


def z_coarsen():
    lane, cell = grid2(LANES, LANES)
    step = lane - ZOFF - 2 * cell
    w = jnp.where((step == 0) | (step == 1), 0.375, jnp.where((step == -1) | (step == 2), 0.125, 0.0))
    return jnp.where(cell < BZ, w, 0.0).astype(BF16)


def z_pick(core):
    lane, y = grid2(BY * BZ, LANES)
    return jnp.where(lane == BZ * y + jnp.where(core == 0, BZ - 1, 0), 1.0, 0.0).astype(BF16)


def z_spread(core):
    y, lane = grid2(LANES, BY * BZ)
    return jnp.where(lane == BZ * y + jnp.where(core == 0, BZ - 1, 0), -0.5, 0.0).astype(BF16)


def stencil(first, columns):
    source, lane = grid2(4 * LANES, columns)
    step = source - LANES - lane
    z = (lax.broadcasted_iota(jnp.int32, (1, columns), 1) + first) % BZ
    up = jnp.where(z == BZ - 1, 2 * BY * BZ, 1)
    down = jnp.where(z == 0, 2 * BY * BZ, -1)
    near = (step == up) | (step == down) | (step == BZ) | (step == -BZ)
    return jnp.where(near, -0.5, jnp.where(step == 0, 3.0, 0.0)).astype(BF16)


def sum_rows(value):
    while value.shape[0] % 16 == 0:
        half = value.shape[0] // 2
        value = value[:half] + value[half:]
    return jnp.sum(value, axis=0, keepdims=True)


def density_kernel(counts, orb, occ, part, held, zf, *refs):
    x_faces, (weights, load, load_occ) = refs[:-3], refs[-3:]
    planes, bands, width = held.shape
    tiles = width // LANES
    pos = position(counts)
    first = pltpu.make_async_copy(occ, weights, load_occ)
    first.start()
    loads = [pltpu.make_async_copy(orb.at[x], held.at[x], load.at[x]) for x in range(planes)]
    for copy in loads:
        copy.start()
    pick = z_pick(pos[2])
    first.wait()
    rows = jnp.broadcast_to(weights[...], (LANES, bands))
    rows = jnp.concatenate([rows, jnp.zeros((LANES, -bands % LANES), F32)], 1)
    weight = jnp.concatenate([rows[:, b : b + LANES].T for b in range(0, bands, LANES)], 0)[:bands]
    for x in range(planes):
        loads[x].wait()
        for t in range(tiles):
            f = held[x, :, t * LANES : (t + 1) * LANES].astype(F32)
            part[tiles * x + t : tiles * x + t + 1, :] = sum_rows(f * f * weight)
        zf[x] = jnp.dot(held[x], pick, preferred_element_type=F32).astype(BF16)
    for side, face in zip(sides(counts[0]), x_faces):
        face[...] = held[rim_start(side, pos[0], planes, 1)]


def total_kernel(counts, scale, *refs):
    parts, out, flat = refs[:-2], refs[-2], refs[-1]
    total = parts[0][...]
    for part in parts[1:]:
        total = total + part[...]
    flat[...] = total * scale
    per = 384 // BZ
    groups = flat.shape[0] // 3
    lane = lane_iota(groups)
    shift = jnp.where(position(counts)[2] == 0, 0, BZ)
    tile = [flat[pl.ds(j, groups, stride=3), :] for j in range(3)]
    for k in range(per):
        at, off = divmod(BZ * k, LANES)
        row = pltpu.roll(tile[at], (LANES - off) % LANES, 1) if off else tile[at]
        if off + BZ > LANES:
            row = jnp.where(lane < LANES - off, row, pltpu.roll(tile[at + 1], LANES - off, 1))
        row = jnp.where(lane < BZ, row, 0.0)
        out[pl.ds(k, groups, stride=per), :] = pltpu.roll(row, shift, 1)


def cut_kernel(counts, rho, mate, chip, *sends):
    cx, cy, _ = position(counts)
    chip[...] = rho[...] + mate[...]
    sends = list(sends)
    x_sides, y_sides = sides(counts[0]), sides(counts[1])
    bx = chip.shape[0] // BY
    for side in x_sides:
        at = pl.multiple_of(BY * rim_start(side, cx, bx, WC), 8)
        sends.pop(0)[...] = chip[pl.ds(at, WC * BY), :].astype(BF16)
    for side in y_sides:
        at = rim_start(side, cy, BY, PAD)
        rows = [chip[pl.ds(pl.multiple_of(BY * x + at, 8), PAD), :] for x in range(bx)]
        sends.pop(0)[...] = jnp.concatenate(rows, 0).astype(BF16)
    for x_side in x_sides:
        for y_side in y_sides:
            at_x, at = rim_start(x_side, cx, bx, WC), rim_start(y_side, cy, BY, PAD)
            rows = [chip[pl.ds(pl.multiple_of(BY * (at_x + x) + at, 8), PAD), :] for x in range(WC)]
            rows.append(jnp.zeros((PAD, LANES), F32))
            sends.pop(0)[...] = jnp.concatenate(rows, 0).astype(BF16)


def field_rows(ref, groups):
    lane = lane_iota(groups)
    a, b, c = (ref[pl.ds(j, groups, stride=3), :] for j in range(3))
    return (
        pltpu.roll(a, 16, 1),
        jnp.where(lane < 48, pltpu.roll(a, 48, 1), pltpu.roll(b, 48, 1)),
        jnp.where(lane < 80, pltpu.roll(b, 80, 1), pltpu.roll(c, 80, 1)),
        pltpu.roll(c, 112, 1),
    )


def field_kernel(counts, orb, prev, comp, mate_prev, mate_comp, ext, *refs):
    sends, pos = list(refs), position(counts)
    bx, bands, row_lanes = orb.shape
    half = bands // 2
    fx, fy = prev.shape[0] * LANES // (2 * BY * 2 * BZ), 2 * BY
    groups = prev.shape[0] // 3
    lane = lane_iota(groups)
    own = (lane >= ZOFF) & (lane < ZOFF + 2 * BZ)
    first = pos[2] == 0
    shift = jnp.where(first, 2 * BZ, LANES - 2 * BZ)
    edge_low = jnp.where(first, ZOFF + 2 * BZ, 0)
    edge_high = jnp.where(first, LANES, ZOFF)
    edge = (lane >= edge_low) & (lane < edge_high)
    rows = fx * fy
    for f, (ref, mate) in enumerate(((prev, mate_prev), (comp, mate_comp))):
        mine = field_rows(ref, groups)
        theirs = field_rows(mate, groups)
        for k in range(4):
            halo = jnp.where(edge, pltpu.roll(theirs[k], shift, 1), 0.0)
            ext[pl.ds(f * rows + k, groups, stride=4), :] = jnp.where(own, mine[k], halo)
    widths = (WV, WS)
    x_sides, y_sides = sides(counts[0]), sides(counts[1])
    for side in x_sides:
        send, done = sends.pop(0), 0
        for f, width in enumerate(widths):
            start = f * rows + fy * rim_start(side, pos[0], fx, width)
            send[pl.ds(done, width * fy), :] = ext[pl.ds(pl.multiple_of(start, 8), width * fy), :].astype(BF16)
            done += width * fy
    first_half = lane_iota(half) < BZ
    for side in y_sides:
        send = sends.pop(0)
        start = pl.multiple_of(rim_start(side, pos[1], row_lanes, LANES), LANES)
        turn = jnp.where(pos[1] == 0, BZ, 0) if side == "swap" else (BZ if side == "lo" else 0)
        for x in range(bx):
            face = orb[x, :, pl.ds(start, LANES)].astype(F32)
            both = jnp.where(first_half, pltpu.roll(face[:half], turn, 1), pltpu.roll(face[half:], turn + BZ, 1))
            send[pl.ds(x * half, half), :] = both.astype(BF16)
        at = rim_start(side, pos[1], fy, PAD)
        for f in range(2):
            cut = [ext[pl.ds(pl.multiple_of(f * rows + fy * x + at, 8), PAD), :] for x in range(fx)]
            send[pl.ds(bx * half + f * fx * PAD, fx * PAD), :] = jnp.concatenate(cut, 0).astype(BF16)
    for x_side in x_sides:
        for y_side in y_sides:
            send = sends.pop(0)
            at = rim_start(y_side, pos[1], fy, PAD)
            cut = []
            for f, width in enumerate(widths):
                start = rim_start(x_side, pos[0], fx, width)
                cut += [
                    ext[pl.ds(pl.multiple_of(f * rows + fy * (start + x) + at, 8), PAD), :]
                    for x in range(width)
                ]
            cut.append(jnp.zeros((PAD, LANES), F32))
            send[...] = jnp.concatenate(cut, 0).astype(BF16)


def finish_kernel(counts, *refs):
    it = iter(refs)
    chip, ext, local_potential, orb, inner, zf = (next(it) for _ in range(6))
    x_sides, y_sides = sides(counts[0]), sides(counts[1])
    xy_sides = [(a, b) for a in x_sides for b in y_sides]
    rho_x, rho_y, rho_xy = ([next(it) for _ in s] for s in (x_sides, y_sides, xy_sides))
    fld_x, fld_y, fld_xy = ([next(it) for _ in s] for s in (x_sides, y_sides, xy_sides))
    x_faces = [next(it) for _ in x_sides]
    out, potential_out = next(it), next(it)
    coarse, wide, fine, v0, v1, src, flat, effective, potential, result, store, store_potential = it
    cx, cy, cz = position(counts)
    bands = orb.shape[1]
    bx = chip.shape[0] // BY
    fx, fy = 2 * bx, 2 * BY
    ry, rc = fy + 2 * PAD, BY + 2 * PAD
    qx = fx + 2 * WV
    face_rows = bx * bands // 2

    coarse[...] = jnp.zeros_like(coarse)
    for x in range(bx):
        coarse[WC + x, PAD : PAD + BY, :] = chip[x * BY : (x + 1) * BY, :]
    for side, ref in zip(x_sides, rho_x):
        at = halo_start(side, cx, 0, WC + bx)
        block = ref[...].astype(F32)
        for x in range(WC):
            coarse[at + x, PAD : PAD + BY, :] = block[x * BY : (x + 1) * BY, :]
    for side, ref in zip(y_sides, rho_y):
        at = pl.multiple_of(halo_start(side, cy, 0, PAD + BY), 8)
        block = ref[...].astype(F32)
        for x in range(bx):
            coarse[WC + x, pl.ds(at, PAD), :] = block[x * PAD : (x + 1) * PAD, :]
    for (x_side, y_side), ref in zip(xy_sides, rho_xy):
        at_x = halo_start(x_side, cx, 0, WC + bx)
        at = pl.multiple_of(halo_start(y_side, cy, 0, PAD + BY), 8)
        block = ref[...].astype(F32)
        for x in range(WC):
            coarse[at_x + x, pl.ds(at, PAD), :] = block[x * PAD : (x + 1) * PAD, :]

    v0[...] = jnp.zeros_like(v0)
    src[...] = jnp.zeros_like(src)
    for f, (ref, width) in enumerate(((v0, WV), (src, WS))):
        rows = f * fx * fy
        for x in range(fx):
            ref[WV + x, PAD : PAD + fy, :] = ext[rows + x * fy : rows + (x + 1) * fy, :]
        done = f * WV
        for side, got in zip(x_sides, fld_x):
            at = halo_start(side, cx, WV - width, WV + fx)
            for x in range(width):
                ref[at + x, PAD : PAD + fy, :] = got[(done + x) * fy : (done + x + 1) * fy, :].astype(F32)
        for side, got in zip(y_sides, fld_y):
            at = pl.multiple_of(halo_start(side, cy, 0, PAD + fy), 8)
            block = got[face_rows + f * fx * PAD : face_rows + (f + 1) * fx * PAD, :].astype(F32)
            for x in range(fx):
                ref[WV + x, pl.ds(at, PAD), :] = block[x * PAD : (x + 1) * PAD, :]
        for (x_side, y_side), got in zip(xy_sides, fld_xy):
            at_x = halo_start(x_side, cx, WV - width, WV + fx)
            at = pl.multiple_of(halo_start(y_side, cy, 0, PAD + fy), 8)
            block = got[...].astype(F32)
            for x in range(width):
                ref[at_x + x, pl.ds(at, PAD), :] = block[(done + x) * PAD : (done + x + 1) * PAD, :]

    cells = (bx + 2 * WC) * rc
    wide[...] = exact_dot(coarse[...].reshape(cells, LANES), z_refine(cz))
    for p in range(bx + 2 * WC):
        base, half = p * rc + PAD // 2, ry // 2
        here = 0.75 * wide[pl.ds(base, half), :]
        fine[pl.ds(p * ry, half, stride=2), :] = here + 0.25 * wide[pl.ds(base - 1, half), :]
        fine[pl.ds(p * ry + 1, half, stride=2), :] = here + 0.25 * wide[pl.ds(base + 1, half), :]
    for q in range(1, qx - 1):
        at = q - WV
        here, other = at // 2 + WC, at // 2 + WC + (1 if at % 2 else -1)
        refined = 0.75 * fine[pl.ds(here * ry, ry), :] + 0.25 * fine[pl.ds(other * ry, ry), :]
        src[q] = math.pi * (refined - src[q])

    row = lax.broadcasted_iota(jnp.int32, (ry, LANES), 0) - PAD + fy * cy
    lane = lane_iota(ry) - ZOFF + 2 * BZ * cz
    inside = (row >= 0) & (row < fy * counts[1]) & (lane >= 0) & (lane < 2 * BZ * counts[2])
    share = jnp.where(inside, 1.0 / 6.0, 0.0)
    old, new = v0, v1
    for sweep in range(SWEEPS):
        for q in range(sweep + 1, qx - sweep - 1):
            at = q - WV + fx * cx
            here = old[q]
            total = old[q - 1] + old[q + 1]
            total = total + pltpu.roll(here, 1, 0) + pltpu.roll(here, ry - 1, 0)
            total = total + pltpu.roll(here, 1, 1) + pltpu.roll(here, LANES - 1, 1)
            total = (total + src[q]) * share
            if q < WV or q >= WV + fx:
                total = jnp.where((at >= 0) & (at < fx * counts[0]), total, 0.0)
            new[q] = total
        old, new = new, old

    groups = fy // 4
    lane = lane_iota(groups)
    for x in range(fx):
        r = [old[WV + x, pl.ds(PAD + k, groups, stride=4), :] for k in range(4)]
        r1, r2 = pltpu.roll(r[1], 80, 1), pltpu.roll(r[2], 48, 1)
        potential[pl.ds(3 * groups * x, groups, stride=3), :] = jnp.where(lane < 96, pltpu.roll(r[0], 112, 1), r1)
        potential[pl.ds(3 * groups * x + 1, groups, stride=3), :] = jnp.where(lane < 64, r1, r2)
        potential[pl.ds(3 * groups * x + 2, groups, stride=3), :] = jnp.where(lane < 32, r2, pltpu.roll(r[3], 16, 1))

    send_potential = pltpu.make_async_copy(potential, potential_out, store_potential)
    send_potential.start()

    pieces = []
    for x in range(bx):
        q = WV + 2 * x
        fine[pl.ds(x * ry, ry), :] = 0.125 * (old[q - 1] + old[q + 2]) + 0.375 * (old[q] + old[q + 1])
        rows = [fine[pl.ds(x * ry + PAD + k, BY, stride=2), :] for k in (-1, 0, 1, 2)]
        pieces.append(0.125 * (rows[0] + rows[3]) + 0.375 * (rows[1] + rows[2]))
    back = exact_dot(jnp.concatenate(pieces, 0), z_coarsen())
    rho = (3.0 / math.pi) * pltpu.roll(chip[...], jnp.where(cz == 0, 0, LANES - BZ), 1)
    safe = jnp.where(rho > 0.0, rho, 1.0)
    root = jnp.exp(jnp.log(safe) * (1.0 / 3.0))
    root = root - (root - safe / (root * root)) * (1.0 / 3.0)
    flat[...] = back - jnp.where(rho > 0.0, root, 0.0)

    per = 384 // BZ
    groups = flat.shape[0] // per
    lane = lane_iota(groups)
    r = [pltpu.roll(flat[pl.ds(k, groups, stride=per), :], BZ * k % LANES, 1) for k in range(per)]
    for j in range(3):
        tile = None
        for k in range(per):
            low, high = BZ * k - LANES * j, BZ * (k + 1) - LANES * j
            if high > 0 and low < LANES:
                tile = r[k] if tile is None else jnp.where(lane >= low, r[k], tile)
        wide[pl.ds(j, groups, stride=3), :] = tile
    tiles = BY * BZ // LANES
    for t in range(tiles):
        cut = slice(t * LANES, (t + 1) * LANES)
        effective[:, cut] = wide[pl.ds(t, bx, stride=tiles), :]
    for x in range(bx):
        effective[x : x + 1, :] = effective[x : x + 1, :] + local_potential[x]

    width, half = effective.shape[1], bands // 2
    spread = z_spread(cz)
    lane = lane_iota(half)
    stores = []
    for x in range(bx):
        outer = jnp.dot(zf[x], spread, preferred_element_type=F32)
        low = high = None
        for side, face in zip(y_sides, fld_y):
            halo = -0.5 * face[x * half : (x + 1) * half, :].astype(F32)
            if side != "hi":
                here = jnp.concatenate([halo, pltpu.roll(halo, LANES - BZ, 1)], 0)
                keep = jnp.concatenate([lane, lane], 0) < BZ
                low = jnp.where(keep & (cy > 0), here, 0.0)
            if side != "lo":
                here = jnp.concatenate([pltpu.roll(halo, LANES - BZ, 1), pltpu.roll(halo, LANES - 2 * BZ, 1)], 0)
                keep = jnp.concatenate([lane, lane], 0) >= LANES - BZ
                high = jnp.where(keep & (cy < counts[1] - 1), here, 0.0)
        for t in range(width // LANES):
            cut = slice(t * LANES, (t + 1) * LANES)
            total = inner[x, :, cut] + outer[:, cut] + effective[x : x + 1, cut] * orb[x, :, cut].astype(F32)
            if t == 0:
                total = total + low
            if t == width // LANES - 1:
                total = total + high
            for side, face in zip(x_sides, x_faces):
                if x == 0 and side != "hi":
                    total = total + jnp.where(cx > 0, -0.5, 0.0) * face[:, cut].astype(F32)
                if x == bx - 1 and side != "lo":
                    total = total + jnp.where(cx < counts[0] - 1, -0.5, 0.0) * face[:, cut].astype(F32)
            result[x, :, cut] = total.astype(BF16)
        stores.append(pltpu.make_async_copy(result.at[x], out.at[x], store.at[x]))
        stores[-1].start()
    for copy in stores + [send_potential]:
        copy.wait()


def laplace_kernel(orb, out):
    planes, bands, width = orb.shape
    step = 2 * LANES
    weights = [stencil(step * p % BZ, step) for p in range(3)]
    for j in range(0, width, step):
        columns = min(step, width - j)
        first, last = max(j - LANES, 0), min(j + step + LANES, width)
        skip = first - (j - LANES)
        w = weights[j // step % 3][skip : skip + last - first, :columns]
        here = orb[:, :, first:last].reshape(planes * bands, last - first)
        total = jnp.dot(here, w, preferred_element_type=F32).reshape(planes, bands, columns)
        for x in range(planes):
            near = [orb[n, :, j : j + columns].astype(F32) for n in (x - 1, x + 1) if 0 <= n < planes]
            out[x, :, j : j + columns] = total[x] - 0.5 * sum(near)


def vmem():
    return pl.BlockSpec(memory_space=pltpu.VMEM)


def local(mesh, orbitals, occupations, previous, compensation, local_potential):
    return step(mesh, orbitals, occupations, previous, compensation, local_potential)


def step(mesh, orbitals, occupations, previous, compensation, local_potential):
    domains, groups = mesh.shape["dom"], mesh.shape["band"]
    split_z = 2
    split_y = min(4, domains // 4)
    counts = (domains // (split_y * split_z), split_y, split_z)
    bands, _, bx, width = orbitals.shape
    tiles = width // LANES
    fx, fy = 2 * bx, 2 * BY
    x_sides, y_sides = sides(counts[0]), sides(counts[1])
    xy_sides = [(a, b) for a in x_sides for b in y_sides]
    moves = [{0: s} for s in x_sides] + [{1: s} for s in y_sides] + [{0: a, 1: b} for a, b in xy_sides]
    hbm = pl.BlockSpec(memory_space=pltpu.HBM)

    def shape(*dims, dtype=F32):
        return jax.ShapeDtypeStruct(dims, dtype)

    def params(kib):
        return pltpu.CompilerParams(vmem_limit_bytes=kib * 2**10)

    flat = [a.reshape(fx * fy * 2 * BZ // LANES, LANES) for a in (previous, compensation)]
    mates = [fetch(a, counts, {2: "swap"}) for a in flat]

    orb = jnp.transpose(orbitals.reshape(bands, bx, width), (1, 0, 2))
    part, orb, z_face, *x_faces = pl.pallas_call(
        functools.partial(density_kernel, counts),
        in_specs=[hbm, hbm],
        out_specs=[vmem()] * (3 + len(x_sides)),
        out_shape=[shape(bx * tiles, LANES), shape(*orb.shape, dtype=BF16), shape(bx, bands, LANES, dtype=BF16)]
        + [shape(bands, width, dtype=BF16) for _ in x_sides],
        scratch_shapes=[pltpu.VMEM((1, bands), F32), pltpu.SemaphoreType.DMA((bx,)), pltpu.SemaphoreType.DMA(())],
        compiler_params=params(8 * 1024),
        name="density",
    )(
        pltpu.with_memory_space_constraint(orb, pltpu.HBM),
        pltpu.with_memory_space_constraint(occupations.reshape(1, bands), pltpu.HBM),
    )
    x_faces = [fetch(f, counts, {0: s}) for s, f in zip(x_sides, x_faces)]
    parts = [part]
    for shift in range(1, groups):
        route = [(i, (i + shift) % groups) for i in range(groups)]
        parts.append(lax.ppermute(part, "band", route))
    z_face = fetch(z_face, counts, {2: "swap"})

    inner = pl.pallas_call(
        laplace_kernel,
        in_specs=[vmem()],
        out_specs=vmem(),
        out_shape=shape(bx, bands, width),
        compiler_params=params(16 * 1024),
        cost_estimate=pl.CostEstimate(flops=6 * 10**9, bytes_accessed=8 * 10**6, transcendentals=0),
        name="laplace",
    )(orb)

    rim_rows = [(WV + WS) * fy] * len(x_sides) + [bx * bands // 2 + 2 * fx * PAD] * len(y_sides)
    rim_rows += [(WV + WS + 1) * PAD] * len(xy_sides)
    ext, *rims = pl.pallas_call(
        functools.partial(field_kernel, counts),
        in_specs=[vmem()] * 5,
        out_specs=[vmem()] * (1 + len(rim_rows)),
        out_shape=[shape(2 * fx * fy, LANES)] + [shape(n, LANES, dtype=BF16) for n in rim_rows],
        compiler_params=params(4 * 1024),
        cost_estimate=pl.CostEstimate(flops=3 * 10**9, bytes_accessed=10**6, transcendentals=0),
        name="fields",
    )(orb, *flat, *mates)
    fields = [fetch(r, counts, m) for r, m in zip(rims, moves)]

    rho = pl.pallas_call(
        functools.partial(total_kernel, counts, 1.0 / (bands * groups)),
        in_specs=[vmem()] * groups,
        out_specs=vmem(),
        out_shape=shape(bx * BY, LANES),
        scratch_shapes=[pltpu.VMEM((bx * tiles, LANES), F32)],
        compiler_params=params(1024),
        name="total",
    )(*parts)
    mate = fetch(rho, counts, {2: "swap"})
    cut_rows = [WC * BY] * len(x_sides) + [bx * PAD] * len(y_sides) + [(WC + 1) * PAD] * len(xy_sides)
    chip, *cuts = pl.pallas_call(
        functools.partial(cut_kernel, counts),
        in_specs=[vmem(), vmem()],
        out_specs=[vmem()] * (1 + len(cut_rows)),
        out_shape=[shape(bx * BY, LANES)] + [shape(n, LANES, dtype=BF16) for n in cut_rows],
        compiler_params=params(1024),
        name="cut",
    )(rho, mate)
    densities = [fetch(c, counts, m) for c, m in zip(cuts, moves)]

    rc, ry, qx = BY + 2 * PAD, fy + 2 * PAD, fx + 2 * WV
    local_rows = jnp.transpose(local_potential, (1, 0, 2))
    operands = [chip, ext, local_rows, orb, inner, z_face, *densities, *fields, *x_faces]
    applied, potential = pl.pallas_call(
        functools.partial(finish_kernel, counts),
        in_specs=[vmem()] * len(operands),
        out_specs=[hbm, hbm],
        scratch_shapes=[
            pltpu.VMEM((bx + 2 * WC, rc, LANES), F32),
            pltpu.VMEM(((bx + 2 * WC) * rc, LANES), F32),
            pltpu.VMEM(((bx + 2 * WC) * ry, LANES), F32),
            pltpu.VMEM((qx, ry, LANES), F32),
            pltpu.VMEM((qx, ry, LANES), F32),
            pltpu.VMEM((qx, ry, LANES), F32),
            pltpu.VMEM((bx * BY, LANES), F32),
            pltpu.VMEM((bx, width), F32),
            pltpu.VMEM(flat[0].shape, F32),
            pltpu.VMEM((bx, bands, width), BF16),
            pltpu.SemaphoreType.DMA((bx,)),
            pltpu.SemaphoreType.DMA(()),
        ],
        out_shape=[shape(bx, bands, width, dtype=BF16), shape(*flat[0].shape)],
        compiler_params=params(20 * 1024),
        name="finish",
    )(*operands)
    applied = jnp.transpose(applied, (1, 0, 2)).reshape(orbitals.shape)
    return applied, potential.reshape(previous.shape)


def solution(mesh):
    return jax.shard_map(
        functools.partial(local, mesh),
        mesh=mesh,
        in_specs=(
            P("band", "dom", None, None),
            P("band"),
            P("dom", None, None),
            P("dom", None, None),
            P("dom", None, None),
        ),
        out_specs=(P("band", "dom", None, None), P("dom", None, None)),
        check_vma=False,
    )
```

```python
import functools
import math

import jax
import jax.numpy as jnp
import numpy as np
from jax import lax
from jax.experimental import pallas as pl
from jax.experimental.pallas import tpu as pltpu
from jax.sharding import PartitionSpec as P


BY = 24
BZ = 48
SWEEPS = 4

F32, BF16 = jnp.float32, jnp.bfloat16
LANES = 128
PAD = 8
ZOFF = 16
WV = SWEEPS + 1
WS = SWEEPS
WC = WS // 2 + 1


def sides(count):
    return ("swap",) if count == 2 else ("lo", "hi")


def fetch(block, counts, moves):
    pairs = []
    for target in np.ndindex(*counts):
        source = list(target)
        for axis, side in moves.items():
            source[axis] = {"swap": 1 - target[axis], "lo": target[axis] - 1, "hi": target[axis] + 1}[side]
        if all(0 <= s < n for s, n in zip(source, counts)):
            pairs.append((int(np.ravel_multi_index(source, counts)), int(np.ravel_multi_index(target, counts))))
    return lax.ppermute(block, "dom", pairs)


def rim_start(side, coord, length, width):
    if side == "swap":
        return jnp.where(coord == 0, length - width, 0)
    return length - width if side == "lo" else 0


def halo_start(side, coord, low, high):
    if side == "swap":
        return jnp.where(coord == 0, high, low)
    return low if side == "lo" else high


def position(counts):
    at = lax.axis_index("dom")
    return at // (counts[1] * counts[2]), at // counts[2] % counts[1], at % counts[2]


def lane_iota(rows):
    return lax.broadcasted_iota(jnp.int32, (rows, LANES), 1)


def halves(value):
    high = value.astype(BF16)
    return jnp.concatenate([high, (value - high.astype(F32)).astype(BF16)], 1)


def wide_dot(value, weights):
    return jnp.dot(halves(value), jnp.concatenate([weights, weights], 0), preferred_element_type=F32)


def grid2(rows, columns):
    shape = (rows, columns)
    return (lax.broadcasted_iota(jnp.int32, shape, d) for d in (0, 1))


def z_refine(core):
    cell, lane = grid2(LANES, LANES)
    fine = lane - ZOFF + 2 * BZ * core
    here = fine >> 1
    other = here + 2 * (fine & 1) - 1
    return jnp.where(cell == here, 0.75, jnp.where(cell == other, 0.25, 0.0)).astype(BF16)


def z_coarsen():
    lane, cell = grid2(LANES, LANES)
    step = lane - ZOFF - 2 * cell
    w = jnp.where((step == 0) | (step == 1), 0.375, jnp.where((step == -1) | (step == 2), 0.125, 0.0))
    return jnp.where(cell < BZ, w, 0.0).astype(BF16)


def z_neighbours():
    source, lane = grid2(LANES, LANES)
    step = source - lane
    return jnp.where((step == 1) | (step == -1), 1.0, 0.0).astype(BF16)


def z_pick(core, lanes):
    lane, y = grid2(lanes, LANES)
    return jnp.where(lane == BZ * y + jnp.where(core == 0, BZ - 1, 0), 1.0, 0.0).astype(BF16)


def z_spread(core):
    y, lane = grid2(LANES, BY * BZ)
    return jnp.where(lane == BZ * y + jnp.where(core == 0, BZ - 1, 0), -0.5, 0.0).astype(BF16)


def lanes_of(value, index):
    return jnp.take_along_axis(value, index, axis=1, mode="promise_in_bounds")


def stencil(first, columns):
    source, lane = grid2(4 * LANES, columns)
    step = source - LANES - lane
    z = (lax.broadcasted_iota(jnp.int32, (1, columns), 1) + first) % BZ
    up = jnp.where(z == BZ - 1, 2 * BY * BZ, 1)
    down = jnp.where(z == 0, 2 * BY * BZ, -1)
    near = (step == up) | (step == down) | (step == BZ) | (step == -BZ)
    return jnp.where(near, -0.5, jnp.where(step == 0, 3.0, 0.0)).astype(BF16)


def sum_rows(value):
    while value.shape[0] % 16 == 0:
        half = value.shape[0] // 2
        value = value[:half] + value[half:]
    return jnp.sum(value, axis=0, keepdims=True)


def density_kernel(counts, orb, occ, part, held, zf, *refs):
    x_faces, (weights, load, load_occ) = refs[:-3], refs[-3:]
    planes, bands, width = held.shape
    tiles = width // LANES
    pos = position(counts)
    first = pltpu.make_async_copy(occ, weights, load_occ)
    first.start()
    loads = [pltpu.make_async_copy(orb.at[x], held.at[x], load.at[x]) for x in range(planes)]
    for copy in loads:
        copy.start()
    split = min(4, tiles)
    pick = z_pick(pos[2], split * LANES)
    face_lane = lane_iota(bands) * BZ + jnp.where(pos[2] == 0, BZ - 1, 0)
    first.wait()
    rows = jnp.broadcast_to(weights[...], (LANES, bands))
    rows = jnp.concatenate([rows, jnp.zeros((LANES, -bands % LANES), F32)], 1)
    weight = jnp.concatenate([rows[:, b : b + LANES].T for b in range(0, bands, LANES)], 0)[:bands]
    for x in range(planes):
        loads[x].wait()
        face = jnp.dot(held[x, :, : split * LANES], pick, preferred_element_type=F32)
        for t in range(tiles):
            f = held[x, :, t * LANES : (t + 1) * LANES].astype(F32)
            part[tiles * x + t : tiles * x + t + 1, :] = sum_rows(f * f * weight)
            if t >= split:
                at = face_lane - t * LANES
                face = jnp.where(at >= 0, lanes_of(f, at & (LANES - 1)), face)
        zf[x] = face.astype(BF16)
    for side, face in zip(sides(counts[0]), x_faces):
        face[...] = held[rim_start(side, pos[0], planes, 1)]


def total_kernel(counts, scale, *refs):
    parts, out, flat = refs[:-2], refs[-2], refs[-1]
    total = parts[0][...]
    for part in parts[1:]:
        total = total + part[...]
    flat[...] = total * scale
    per = 384 // BZ
    groups = flat.shape[0] // 3
    lane = lane_iota(groups)
    shift = jnp.where(position(counts)[2] == 0, 0, BZ)
    tile = [flat[pl.ds(j, groups, stride=3), :] for j in range(3)]
    for k in range(per):
        at, off = divmod(BZ * k, LANES)
        row = pltpu.roll(tile[at], (LANES - off) % LANES, 1) if off else tile[at]
        if off + BZ > LANES:
            row = jnp.where(lane < LANES - off, row, pltpu.roll(tile[at + 1], LANES - off, 1))
        row = jnp.where(lane < BZ, row, 0.0)
        out[pl.ds(k, groups, stride=per), :] = pltpu.roll(row, shift, 1)


def cut_kernel(counts, rho, mate, *refs):
    x_sides, y_sides = sides(counts[0]), sides(counts[1])
    corners = len(x_sides) * len(y_sides)
    fields, chip, sends = list(refs[:corners]), refs[corners], list(refs[corners + 1 :])
    cx, cy, _ = position(counts)
    chip[...] = rho[...] + mate[...]
    bx = chip.shape[0] // BY
    for side in x_sides:
        at = pl.multiple_of(BY * rim_start(side, cx, bx, WC), 8)
        sends.pop(0)[...] = chip[pl.ds(at, WC * BY), :].astype(BF16)
    for side in y_sides:
        at = rim_start(side, cy, BY, PAD)
        rows = [chip[pl.ds(pl.multiple_of(BY * x + at, 8), PAD), :] for x in range(bx)]
        sends.pop(0)[...] = jnp.concatenate(rows, 0).astype(BF16)
    for x_side in x_sides:
        for y_side in y_sides:
            at_x, at = rim_start(x_side, cx, bx, WC), rim_start(y_side, cy, BY, PAD)
            rows = [chip[pl.ds(pl.multiple_of(BY * (at_x + x) + at, 8), PAD), :] for x in range(WC)]
            rows.append(jnp.zeros((PAD, LANES), F32))
            rows = jnp.concatenate(rows, 0).astype(BF16)
            sends.pop(0)[...] = jnp.concatenate([rows, fields.pop(0)[...]], 0)


def field_rows(ref, groups):
    lane = lane_iota(groups)
    a, b, c = (ref[pl.ds(j, groups, stride=3), :] for j in range(3))
    return (
        pltpu.roll(a, 16, 1),
        jnp.where(lane < 48, pltpu.roll(a, 48, 1), pltpu.roll(b, 48, 1)),
        jnp.where(lane < 80, pltpu.roll(b, 80, 1), pltpu.roll(c, 80, 1)),
        pltpu.roll(c, 112, 1),
    )


def field_kernel(counts, orb, prev, comp, mate_prev, mate_comp, ext, *refs):
    sends, pos = list(refs), position(counts)
    bx, bands, row_lanes = orb.shape
    half = bands // 2
    fx, fy = prev.shape[0] * LANES // (2 * BY * 2 * BZ), 2 * BY
    groups = prev.shape[0] // 3
    lane = lane_iota(groups)
    own = (lane >= ZOFF) & (lane < ZOFF + 2 * BZ)
    first = pos[2] == 0
    shift = jnp.where(first, 2 * BZ, LANES - 2 * BZ)
    edge_low = jnp.where(first, ZOFF + 2 * BZ, 0)
    edge_high = jnp.where(first, LANES, ZOFF)
    edge = (lane >= edge_low) & (lane < edge_high)
    rows = fx * fy
    for f, (ref, mate) in enumerate(((prev, mate_prev), (comp, mate_comp))):
        mine = field_rows(ref, groups)
        theirs = field_rows(mate, groups)
        for k in range(4):
            halo = jnp.where(edge, pltpu.roll(theirs[k], shift, 1), 0.0)
            ext[pl.ds(f * rows + k, groups, stride=4), :] = jnp.where(own, mine[k], halo)
    widths = (WV, WS)
    x_sides, y_sides = sides(counts[0]), sides(counts[1])
    for side in x_sides:
        send, done = sends.pop(0), 0
        for f, width in enumerate(widths):
            start = f * rows + fy * rim_start(side, pos[0], fx, width)
            send[pl.ds(done, width * fy), :] = ext[pl.ds(pl.multiple_of(start, 8), width * fy), :].astype(BF16)
            done += width * fy
    first_half = lane_iota(half) < BZ
    for side in y_sides:
        send = sends.pop(0)
        start = pl.multiple_of(rim_start(side, pos[1], row_lanes, LANES), LANES)
        turn = jnp.where(pos[1] == 0, BZ, 0) if side == "swap" else (BZ if side == "lo" else 0)
        for x in range(bx):
            face = orb[x, :, pl.ds(start, LANES)].astype(F32)
            both = jnp.where(first_half, pltpu.roll(face[:half], turn, 1), pltpu.roll(face[half:], turn + BZ, 1))
            send[pl.ds(x * half, half), :] = both.astype(BF16)
        at = rim_start(side, pos[1], fy, PAD)
        for f in range(2):
            cut = [ext[pl.ds(pl.multiple_of(f * rows + fy * x + at, 8), PAD), :] for x in range(fx)]
            send[pl.ds(bx * half + f * fx * PAD, fx * PAD), :] = jnp.concatenate(cut, 0).astype(BF16)
    for x_side in x_sides:
        for y_side in y_sides:
            send = sends.pop(0)
            at = rim_start(y_side, pos[1], fy, PAD)
            cut = []
            for f, width in enumerate(widths):
                start = rim_start(x_side, pos[0], fx, width)
                cut += [
                    ext[pl.ds(pl.multiple_of(f * rows + fy * (start + x) + at, 8), PAD), :]
                    for x in range(width)
                ]
            cut.append(jnp.zeros((PAD, LANES), F32))
            send[...] = jnp.concatenate(cut, 0).astype(BF16)


def merge_rows(flat, joined):
    per = 384 // BZ
    groups = flat.shape[0] // per
    lane = lane_iota(groups)
    r = [pltpu.roll(flat[pl.ds(k, groups, stride=per), :], BZ * k % LANES, 1) for k in range(per)]
    for j in range(3):
        tile = None
        for k in range(per):
            low, high = BZ * k - LANES * j, BZ * (k + 1) - LANES * j
            if high > 0 and low < LANES:
                tile = r[k] if tile is None else jnp.where(lane >= low, r[k], tile)
        joined[pl.ds(j, groups, stride=3), :] = tile
    tiles = BY * BZ // LANES
    planes = flat.shape[0] // BY
    columns = [joined[pl.ds(t, planes, stride=tiles), :] for t in range(tiles)]
    rows = jnp.concatenate(columns, 1)
    return [rows[x : x + 1] for x in range(planes)]


def local_kernel(counts, chip, local_potential, out, flat, joined):
    cz = position(counts)[2]
    rho = (3.0 / math.pi) * pltpu.roll(chip[...], jnp.where(cz == 0, 0, LANES - BZ), 1)
    safe = jnp.where(rho > 0.0, rho, 1.0)
    root = jnp.exp(jnp.log(safe) * (1.0 / 3.0))
    root = root - (root - safe / (root * root)) * (1.0 / 3.0)
    flat[...] = jnp.where(rho > 0.0, root, 0.0)
    for x, row in enumerate(merge_rows(flat, joined)):
        out[x : x + 1, :] = local_potential[x] - row


def finish_kernel(counts, *refs):
    it = iter(refs)
    chip, ext, local_part, orb, inner, zf = (next(it) for _ in range(6))
    x_sides, y_sides = sides(counts[0]), sides(counts[1])
    xy_sides = [(a, b) for a in x_sides for b in y_sides]
    rho_x, rho_y, rho_xy = ([next(it) for _ in s] for s in (x_sides, y_sides, xy_sides))
    fld_x, fld_y = ([next(it) for _ in s] for s in (x_sides, y_sides))
    x_faces = [next(it) for _ in x_sides]
    out, potential_out = next(it), next(it)
    coarse, wide, fine, v0, v1, src, flat, effective, potential, result, store, store_potential = it
    cx, cy, cz = position(counts)
    bands = orb.shape[1]
    bx = chip.shape[0] // BY
    fx, fy = 2 * bx, 2 * BY
    ry, rc = fy + 2 * PAD, BY + 2 * PAD
    qx = fx + 2 * WV
    face_rows = bx * bands // 2

    coarse[...] = jnp.zeros_like(coarse)
    for x in range(bx):
        coarse[WC + x, PAD : PAD + BY, :] = chip[x * BY : (x + 1) * BY, :]
    for side, ref in zip(x_sides, rho_x):
        at = halo_start(side, cx, 0, WC + bx)
        block = ref[...].astype(F32)
        for x in range(WC):
            coarse[at + x, PAD : PAD + BY, :] = block[x * BY : (x + 1) * BY, :]
    for side, ref in zip(y_sides, rho_y):
        at = pl.multiple_of(halo_start(side, cy, 0, PAD + BY), 8)
        block = ref[...].astype(F32)
        for x in range(bx):
            coarse[WC + x, pl.ds(at, PAD), :] = block[x * PAD : (x + 1) * PAD, :]
    for (x_side, y_side), ref in zip(xy_sides, rho_xy):
        at_x = halo_start(x_side, cx, 0, WC + bx)
        at = pl.multiple_of(halo_start(y_side, cy, 0, PAD + BY), 8)
        block = ref[...].astype(F32)
        for x in range(WC):
            coarse[at_x + x, pl.ds(at, PAD), :] = block[x * PAD : (x + 1) * PAD, :]

    v0[...] = jnp.zeros_like(v0)
    v1[:, 0:PAD, :] = jnp.zeros((qx, PAD, LANES), F32)
    v1[:, ry - PAD : ry, :] = jnp.zeros((qx, PAD, LANES), F32)
    src[...] = jnp.zeros_like(src)
    for f, (ref, width) in enumerate(((v0, WV), (src, WS))):
        rows = f * fx * fy
        for x in range(fx):
            ref[WV + x, PAD : PAD + fy, :] = ext[rows + x * fy : rows + (x + 1) * fy, :]
        done = f * WV
        for side, got in zip(x_sides, fld_x):
            at = halo_start(side, cx, WV - width, WV + fx)
            for x in range(width):
                ref[at + x, PAD : PAD + fy, :] = got[(done + x) * fy : (done + x + 1) * fy, :].astype(F32)
        for side, got in zip(y_sides, fld_y):
            at = pl.multiple_of(halo_start(side, cy, 0, PAD + fy), 8)
            block = got[face_rows + f * fx * PAD : face_rows + (f + 1) * fx * PAD, :].astype(F32)
            for x in range(fx):
                ref[WV + x, pl.ds(at, PAD), :] = block[x * PAD : (x + 1) * PAD, :]
        for (x_side, y_side), got in zip(xy_sides, rho_xy):
            at_x = halo_start(x_side, cx, WV - width, WV + fx)
            at = pl.multiple_of(halo_start(y_side, cy, 0, PAD + fy), 8)
            block = got[(WC + 1) * PAD :, :].astype(F32)
            for x in range(width):
                ref[at_x + x, pl.ds(at, PAD), :] = block[(done + x) * PAD : (done + x + 1) * PAD, :]

    cells = (bx + 2 * WC) * rc
    wide[...] = wide_dot(coarse[...].reshape(cells, LANES), z_refine(cz))
    for p in range(bx + 2 * WC):
        base, half = p * rc + PAD // 2, ry // 2
        here = 0.75 * wide[pl.ds(base, half), :]
        fine[pl.ds(p * ry, half, stride=2), :] = here + 0.25 * wide[pl.ds(base - 1, half), :]
        fine[pl.ds(p * ry + 1, half, stride=2), :] = here + 0.25 * wide[pl.ds(base + 1, half), :]
    for q in range(1, qx - 1):
        at = q - WV
        here, other = at // 2 + WC, at // 2 + WC + (1 if at % 2 else -1)
        refined = 0.75 * fine[pl.ds(here * ry, ry), :] + 0.25 * fine[pl.ds(other * ry, ry), :]
        src[q] = math.pi * (refined - src[q])

    near, span = PAD - WS, fy + 2 * WS
    row = lax.broadcasted_iota(jnp.int32, (span, LANES), 0) - WS + fy * cy
    lane = lane_iota(span) - ZOFF + 2 * BZ * cz
    inside = (row >= 0) & (row < fy * counts[1]) & (lane >= 0) & (lane < 2 * BZ * counts[2])
    share = jnp.where(inside, 1.0 / 6.0, 0.0)
    old, new = v0, v1
    beside = z_neighbours()
    for sweep in range(SWEEPS):
        first, last = sweep + 1, qx - sweep - 1
        rows = old[first:last, near : near + span, :].reshape((last - first) * span, LANES)
        along_z = wide_dot(rows, beside)
        for q in range(first, last):
            at = q - WV + fx * cx
            total = along_z[(q - first) * span : (q - first + 1) * span]
            total = total + old[q - 1, near : near + span, :] + old[q + 1, near : near + span, :]
            total = total + old[q, near - 1 : near - 1 + span, :] + old[q, near + 1 : near + 1 + span, :]
            total = (total + src[q, near : near + span, :]) * share
            if q < WV or q >= WV + fx:
                total = jnp.where((at >= 0) & (at < fx * counts[0]), total, 0.0)
            new[q, near : near + span, :] = total
        old, new = new, old

    groups = fy // 4
    lane = lane_iota(groups)
    for x in range(fx):
        r = [old[WV + x, pl.ds(PAD + k, groups, stride=4), :] for k in range(4)]
        r1, r2 = pltpu.roll(r[1], 80, 1), pltpu.roll(r[2], 48, 1)
        potential[pl.ds(3 * groups * x, groups, stride=3), :] = jnp.where(lane < 96, pltpu.roll(r[0], 112, 1), r1)
        potential[pl.ds(3 * groups * x + 1, groups, stride=3), :] = jnp.where(lane < 64, r1, r2)
        potential[pl.ds(3 * groups * x + 2, groups, stride=3), :] = jnp.where(lane < 32, r2, pltpu.roll(r[3], 16, 1))

    send_potential = pltpu.make_async_copy(potential, potential_out, store_potential)
    send_potential.start()

    pieces = []
    for x in range(bx):
        q = WV + 2 * x
        fine[pl.ds(x * ry, ry), :] = 0.125 * (old[q - 1] + old[q + 2]) + 0.375 * (old[q] + old[q + 1])
        rows = [fine[pl.ds(x * ry + PAD + k, BY, stride=2), :] for k in (-1, 0, 1, 2)]
        pieces.append(0.125 * (rows[0] + rows[3]) + 0.375 * (rows[1] + rows[2]))
    back = wide_dot(jnp.concatenate(pieces, 0), z_coarsen())
    flat[...] = back
    for x, row in enumerate(merge_rows(flat, wide)):
        effective[x : x + 1, :] = row + local_part[x : x + 1, :]

    width, half = effective.shape[1], bands // 2
    lane = lane_iota(half)
    lane = jnp.concatenate([lane, lane], 0)
    spread = z_spread(cz)
    z_faces = zf[...].reshape(bx * bands, LANES)
    step = 2 * LANES
    stores = []
    for j in range(0, width, step):
        columns = min(step, width - j)
        outer = jnp.dot(z_faces, spread[:, j : j + columns], preferred_element_type=F32)
        for x in range(bx):
            for t in range(j, j + columns, LANES):
                cut = slice(t, t + LANES)
                total = inner[x, :, cut] + effective[x : x + 1, cut] * orb[x, :, cut].astype(F32)
                total = total + outer[x * bands : (x + 1) * bands, t - j : t - j + LANES]
                for side, face in zip(y_sides, fld_y):
                    halo = -0.5 * face[x * half : (x + 1) * half, :].astype(F32)
                    if t == 0 and side != "hi":
                        here = jnp.concatenate([halo, pltpu.roll(halo, LANES - BZ, 1)], 0)
                        total = total + jnp.where((lane < BZ) & (cy > 0), here, 0.0)
                    if t == width - LANES and side != "lo":
                        here = [pltpu.roll(halo, LANES - BZ, 1), pltpu.roll(halo, LANES - 2 * BZ, 1)]
                        keep = (lane >= LANES - BZ) & (cy < counts[1] - 1)
                        total = total + jnp.where(keep, jnp.concatenate(here, 0), 0.0)
                for side, face in zip(x_sides, x_faces):
                    if x == 0 and side != "hi":
                        total = total + jnp.where(cx > 0, -0.5, 0.0) * face[:, cut].astype(F32)
                    if x == bx - 1 and side != "lo":
                        total = total + jnp.where(cx < counts[0] - 1, -0.5, 0.0) * face[:, cut].astype(F32)
                result[x, :, cut] = total.astype(BF16)
        cut = pl.ds(j, columns)
        stores.append(pltpu.make_async_copy(result.at[:, :, cut], out.at[:, :, cut], store.at[j // step]))
        stores[-1].start()
    for copy in stores + [send_potential]:
        copy.wait()


def laplace_kernel(orb, out):
    planes, bands, width = orb.shape
    step = 2 * LANES
    weights = [stencil(step * p % BZ, step) for p in range(3)]
    for j in range(0, width, step):
        columns = min(step, width - j)
        first, last = max(j - LANES, 0), min(j + step + LANES, width)
        skip = first - (j - LANES)
        w = weights[j // step % 3][skip : skip + last - first, :columns]
        here = orb[:, :, first:last].reshape(planes * bands, last - first)
        total = jnp.dot(here, w, preferred_element_type=F32).reshape(planes, bands, columns)
        for x in range(planes):
            near = [orb[n, :, j : j + columns].astype(F32) for n in (x - 1, x + 1) if 0 <= n < planes]
            out[x, :, j : j + columns] = total[x] - 0.5 * sum(near)


def vmem():
    return pl.BlockSpec(memory_space=pltpu.VMEM)


def local(mesh, orbitals, occupations, previous, compensation, local_potential):
    return step(mesh, orbitals, occupations, previous, compensation, local_potential)


def step(mesh, orbitals, occupations, previous, compensation, local_potential):
    domains, groups = mesh.shape["dom"], mesh.shape["band"]
    split_z = 2
    split_y = min(4, domains // 4)
    counts = (domains // (split_y * split_z), split_y, split_z)
    bands, _, bx, width = orbitals.shape
    tiles = width // LANES
    fx, fy = 2 * bx, 2 * BY
    x_sides, y_sides = sides(counts[0]), sides(counts[1])
    xy_sides = [(a, b) for a in x_sides for b in y_sides]
    moves = [{0: s} for s in x_sides] + [{1: s} for s in y_sides] + [{0: a, 1: b} for a, b in xy_sides]
    hbm = pl.BlockSpec(memory_space=pltpu.HBM)

    def shape(*dims, dtype=F32):
        return jax.ShapeDtypeStruct(dims, dtype)

    def params(kib):
        return pltpu.CompilerParams(vmem_limit_bytes=kib * 2**10)

    flat = [a.reshape(fx * fy * 2 * BZ // LANES, LANES) for a in (previous, compensation)]
    mates = [fetch(a, counts, {2: "swap"}) for a in flat]

    orb = jnp.transpose(orbitals.reshape(bands, bx, width), (1, 0, 2))
    part, orb, z_face, *x_faces = pl.pallas_call(
        functools.partial(density_kernel, counts),
        in_specs=[hbm, hbm],
        out_specs=[vmem()] * (3 + len(x_sides)),
        out_shape=[shape(bx * tiles, LANES), shape(*orb.shape, dtype=BF16), shape(bx, bands, LANES, dtype=BF16)]
        + [shape(bands, width, dtype=BF16) for _ in x_sides],
        scratch_shapes=[pltpu.VMEM((1, bands), F32), pltpu.SemaphoreType.DMA((bx,)), pltpu.SemaphoreType.DMA(())],
        compiler_params=params(8 * 1024),
        name="density",
    )(
        pltpu.with_memory_space_constraint(orb, pltpu.HBM),
        pltpu.with_memory_space_constraint(occupations.reshape(1, bands), pltpu.HBM),
    )
    x_faces = [fetch(f, counts, {0: s}) for s, f in zip(x_sides, x_faces)]
    parts = [part]
    for shift in range(1, groups):
        route = [(i, (i + shift) % groups) for i in range(groups)]
        parts.append(lax.ppermute(part, "band", route))
    z_face = fetch(z_face, counts, {2: "swap"})

    inner = pl.pallas_call(
        laplace_kernel,
        in_specs=[vmem()],
        out_specs=vmem(),
        out_shape=shape(bx, bands, width),
        compiler_params=params(16 * 1024),
        cost_estimate=pl.CostEstimate(flops=6 * 10**9, bytes_accessed=8 * 10**6, transcendentals=0),
        name="laplace",
    )(orb)

    rim_rows = [(WV + WS) * fy] * len(x_sides) + [bx * bands // 2 + 2 * fx * PAD] * len(y_sides)
    rim_rows += [(WV + WS + 1) * PAD] * len(xy_sides)
    ext, *rims = pl.pallas_call(
        functools.partial(field_kernel, counts),
        in_specs=[vmem()] * 5,
        out_specs=[vmem()] * (1 + len(rim_rows)),
        out_shape=[shape(2 * fx * fy, LANES)] + [shape(n, LANES, dtype=BF16) for n in rim_rows],
        compiler_params=params(4 * 1024),
        cost_estimate=pl.CostEstimate(flops=3 * 10**9, bytes_accessed=10**6, transcendentals=0),
        name="fields",
    )(orb, *flat, *mates)
    corner_rims = rims[len(x_sides) + len(y_sides) :]
    fields = [fetch(r, counts, m) for r, m in zip(rims, moves) if list(m) == [0]]
    fields += [fetch(r, counts, m) for r, m in zip(rims, moves) if list(m) == [1]]

    rho = pl.pallas_call(
        functools.partial(total_kernel, counts, 1.0 / (bands * groups)),
        in_specs=[vmem()] * groups,
        out_specs=vmem(),
        out_shape=shape(bx * BY, LANES),
        scratch_shapes=[pltpu.VMEM((bx * tiles, LANES), F32)],
        compiler_params=params(1024),
        name="total",
    )(*parts)
    mate = fetch(rho, counts, {2: "swap"})
    corner_rows = (WC + 1) * PAD + (WV + WS + 1) * PAD
    cut_rows = [WC * BY] * len(x_sides) + [bx * PAD] * len(y_sides) + [corner_rows] * len(xy_sides)
    chip, *cuts = pl.pallas_call(
        functools.partial(cut_kernel, counts),
        in_specs=[vmem()] * (2 + len(corner_rims)),
        out_specs=[vmem()] * (1 + len(cut_rows)),
        out_shape=[shape(bx * BY, LANES)] + [shape(n, LANES, dtype=BF16) for n in cut_rows],
        compiler_params=params(1024),
        name="cut",
    )(rho, mate, *corner_rims)
    densities = [fetch(c, counts, m) for c, m in zip(cuts, moves)]

    rc, ry, qx = BY + 2 * PAD, fy + 2 * PAD, fx + 2 * WV
    local_rows = jnp.transpose(local_potential, (1, 0, 2))
    local_part = pl.pallas_call(
        functools.partial(local_kernel, counts),
        in_specs=[vmem(), vmem()],
        out_specs=vmem(),
        out_shape=shape(bx, width),
        scratch_shapes=[pltpu.VMEM((bx * BY, LANES), F32), pltpu.VMEM((bx * tiles, LANES), F32)],
        compiler_params=params(1024),
        name="local",
    )(chip, local_rows)
    operands = [chip, ext, local_part, orb, inner, z_face, *densities, *fields, *x_faces]
    applied, potential = pl.pallas_call(
        functools.partial(finish_kernel, counts),
        in_specs=[vmem()] * len(operands),
        out_specs=[hbm, hbm],
        scratch_shapes=[
            pltpu.VMEM((bx + 2 * WC, rc, LANES), F32),
            pltpu.VMEM(((bx + 2 * WC) * rc, LANES), F32),
            pltpu.VMEM(((bx + 2 * WC) * ry, LANES), F32),
            pltpu.VMEM((qx, ry, LANES), F32),
            pltpu.VMEM((qx, ry, LANES), F32),
            pltpu.VMEM((qx, ry, LANES), F32),
            pltpu.VMEM((bx * BY, LANES), F32),
            pltpu.VMEM((bx, width), F32),
            pltpu.VMEM(flat[0].shape, F32),
            pltpu.VMEM((bx, bands, width), BF16),
            pltpu.SemaphoreType.DMA((pl.cdiv(width, 2 * LANES),)),
            pltpu.SemaphoreType.DMA(()),
        ],
        out_shape=[shape(bx, bands, width, dtype=BF16), shape(*flat[0].shape)],
        compiler_params=params(20 * 1024),
        name="finish",
    )(*operands)
    applied = jnp.transpose(applied, (1, 0, 2)).reshape(orbitals.shape)
    return applied, potential.reshape(previous.shape)


def solution(mesh):
    return jax.shard_map(
        functools.partial(local, mesh),
        mesh=mesh,
        in_specs=(
            P("band", "dom", None, None),
            P("band"),
            P("dom", None, None),
            P("dom", None, None),
            P("dom", None, None),
        ),
        out_specs=(P("band", "dom", None, None), P("dom", None, None)),
        check_vma=False,
    )
```

```python
import functools
import math

import jax
import jax.numpy as jnp
import numpy as np
from jax import lax
from jax.experimental import pallas as pl
from jax.experimental.pallas import tpu as pltpu
from jax.sharding import PartitionSpec as P


BY = 24
BZ = 48
SWEEPS = 4

F32, BF16 = jnp.float32, jnp.bfloat16
LANES = 128
PAD = 8
ZOFF = 16
WV = SWEEPS + 1
WS = SWEEPS
WC = WS // 2 + 1


def sides(count):
    return ("swap",) if count == 2 else ("lo", "hi")


def fetch(block, counts, moves):
    pairs = []
    for target in np.ndindex(*counts):
        source = list(target)
        for axis, side in moves.items():
            source[axis] = {"swap": 1 - target[axis], "lo": target[axis] - 1, "hi": target[axis] + 1}[side]
        if all(0 <= s < n for s, n in zip(source, counts)):
            pairs.append((int(np.ravel_multi_index(source, counts)), int(np.ravel_multi_index(target, counts))))
    return lax.ppermute(block, "dom", pairs)


def rim_start(side, coord, length, width):
    if side == "swap":
        return jnp.where(coord == 0, length - width, 0)
    return length - width if side == "lo" else 0


def halo_start(side, coord, low, high):
    if side == "swap":
        return jnp.where(coord == 0, high, low)
    return low if side == "lo" else high


def position(counts):
    at = lax.axis_index("dom")
    return at // (counts[1] * counts[2]), at // counts[2] % counts[1], at % counts[2]


def lane_iota(rows):
    return lax.broadcasted_iota(jnp.int32, (rows, LANES), 1)


def halves(value):
    high = value.astype(BF16)
    return jnp.concatenate([high, (value - high.astype(F32)).astype(BF16)], 1)


def wide_dot(value, weights):
    return jnp.dot(halves(value), jnp.concatenate([weights, weights], 0), preferred_element_type=F32)


def grid2(rows, columns):
    shape = (rows, columns)
    return (lax.broadcasted_iota(jnp.int32, shape, d) for d in (0, 1))


def z_refine(core):
    cell, lane = grid2(LANES, LANES)
    fine = lane - ZOFF + 2 * BZ * core
    here = fine >> 1
    other = here + 2 * (fine & 1) - 1
    return jnp.where(cell == here, 0.75, jnp.where(cell == other, 0.25, 0.0)).astype(BF16)


def z_coarsen():
    lane, cell = grid2(LANES, LANES)
    step = lane - ZOFF - 2 * cell
    w = jnp.where((step == 0) | (step == 1), 0.375, jnp.where((step == -1) | (step == 2), 0.125, 0.0))
    return jnp.where(cell < BZ, w, 0.0).astype(BF16)


def z_neighbours():
    source, lane = grid2(LANES, LANES)
    step = source - lane
    return jnp.where((step == 1) | (step == -1), 1.0, 0.0).astype(BF16)


def z_pick(core, lanes):
    lane, y = grid2(lanes, LANES)
    return jnp.where(lane == BZ * y + jnp.where(core == 0, BZ - 1, 0), 1.0, 0.0).astype(BF16)


def z_spread(core):
    y, lane = grid2(LANES, BY * BZ)
    return jnp.where(lane == BZ * y + jnp.where(core == 0, BZ - 1, 0), -0.5, 0.0).astype(BF16)


def lanes_of(value, index):
    pieces = [value[r : r + 8] for r in range(0, value.shape[0], 8)]
    return [jnp.take_along_axis(p, index, axis=1, mode="promise_in_bounds") for p in pieces]


def stencil(first, columns):
    source, lane = grid2(4 * LANES, columns)
    step = source - LANES - lane
    z = (lax.broadcasted_iota(jnp.int32, (1, columns), 1) + first) % BZ
    up = jnp.where(z == BZ - 1, 2 * BY * BZ, 1)
    down = jnp.where(z == 0, 2 * BY * BZ, -1)
    near = (step == up) | (step == down) | (step == BZ) | (step == -BZ)
    return jnp.where(near, -0.5, jnp.where(step == 0, 3.0, 0.0)).astype(BF16)


def sum_rows(value):
    while value.shape[0] % 16 == 0:
        half = value.shape[0] // 2
        value = value[:half] + value[half:]
    return jnp.sum(value, axis=0, keepdims=True)


def density_kernel(counts, orb, occ, prev, comp, part, held, mate_sent, *refs):
    x_faces, (weights, fields, load, load_occ, load_field) = refs[:-5], refs[-5:]
    planes, bands, width = held.shape
    tiles, rows = width // LANES, prev.shape[0]
    pos = position(counts)
    first = pltpu.make_async_copy(occ, weights, load_occ)
    first.start()
    loads = [pltpu.make_async_copy(orb.at[x], held.at[x], load.at[x]) for x in range(planes)]
    loads += [pltpu.make_async_copy(ref, fields.at[f], load_field.at[f]) for f, ref in enumerate((prev, comp))]
    for copy in loads:
        copy.start()
    split = min(4, tiles)
    pick = z_pick(pos[2], split * LANES)
    face_lane = lane_iota(8) * BZ + jnp.where(pos[2] == 0, BZ - 1, 0)
    first.wait()
    column = jnp.broadcast_to(weights[...], (LANES, bands))
    column = jnp.concatenate([column, jnp.zeros((LANES, -bands % LANES), F32)], 1)
    weight = jnp.concatenate([column[:, b : b + LANES].T for b in range(0, bands, LANES)], 0)[:bands]
    for x in range(planes):
        loads[x].wait()
        face = jnp.dot(held[x, :, : split * LANES], pick, preferred_element_type=F32)
        for t in range(tiles):
            f = held[x, :, t * LANES : (t + 1) * LANES].astype(F32)
            part[tiles * x + t : tiles * x + t + 1, :] = sum_rows(f * f * weight)
            if t >= split:
                at = face_lane - t * LANES
                got = lanes_of(f, at & (LANES - 1))
                face = [jnp.where(at >= 0, new, face[8 * i : 8 * i + 8]) for i, new in enumerate(got)]
                face = jnp.concatenate(face, 0)
        mate_sent[2 * rows + x * bands : 2 * rows + (x + 1) * bands, :] = face.astype(BF16)
    for side, face in zip(sides(counts[0]), x_faces):
        face[...] = held[rim_start(side, pos[0], planes, 1)]
    for f in range(2):
        loads[planes + f].wait()
        mate_sent[f * rows : (f + 1) * rows, :] = fields[f].astype(BF16)


def total_kernel(counts, scale, *refs):
    parts, out, flat = refs[:-2], refs[-2], refs[-1]
    total = parts[0][...]
    for part in parts[1:]:
        total = total + part[...]
    flat[...] = total * scale
    per = 384 // BZ
    groups = flat.shape[0] // 3
    lane = lane_iota(groups)
    shift = jnp.where(position(counts)[2] == 0, 0, BZ)
    tile = [flat[pl.ds(j, groups, stride=3), :] for j in range(3)]
    for k in range(per):
        at, off = divmod(BZ * k, LANES)
        row = pltpu.roll(tile[at], (LANES - off) % LANES, 1) if off else tile[at]
        if off + BZ > LANES:
            row = jnp.where(lane < LANES - off, row, pltpu.roll(tile[at + 1], LANES - off, 1))
        row = jnp.where(lane < BZ, row, 0.0)
        out[pl.ds(k, groups, stride=per), :] = pltpu.roll(row, shift, 1)


def cut_kernel(counts, rho, mate, *refs):
    x_sides, y_sides = sides(counts[0]), sides(counts[1])
    corners = len(x_sides) * len(y_sides)
    fields, chip, sends = list(refs[:corners]), refs[corners], list(refs[corners + 1 :])
    cx, cy, _ = position(counts)
    chip[...] = rho[...] + mate[...]
    bx = chip.shape[0] // BY
    for side in x_sides:
        at = pl.multiple_of(BY * rim_start(side, cx, bx, WC), 8)
        sends.pop(0)[...] = chip[pl.ds(at, WC * BY), :].astype(BF16)
    for side in y_sides:
        at = rim_start(side, cy, BY, PAD)
        rows = [chip[pl.ds(pl.multiple_of(BY * x + at, 8), PAD), :] for x in range(bx)]
        sends.pop(0)[...] = jnp.concatenate(rows, 0).astype(BF16)
    for x_side in x_sides:
        for y_side in y_sides:
            at_x, at = rim_start(x_side, cx, bx, WC), rim_start(y_side, cy, BY, PAD)
            rows = [chip[pl.ds(pl.multiple_of(BY * (at_x + x) + at, 8), PAD), :] for x in range(WC)]
            rows.append(jnp.zeros((PAD, LANES), F32))
            rows = jnp.concatenate(rows, 0).astype(BF16)
            sends.pop(0)[...] = jnp.concatenate([rows, fields.pop(0)[...]], 0)


def field_rows(ref, groups):
    lane = lane_iota(groups)
    a, b, c = (ref[pl.ds(j, groups, stride=3), :] for j in range(3))
    return (
        pltpu.roll(a, 16, 1),
        jnp.where(lane < 48, pltpu.roll(a, 48, 1), pltpu.roll(b, 48, 1)),
        jnp.where(lane < 80, pltpu.roll(b, 80, 1), pltpu.roll(c, 80, 1)),
        pltpu.roll(c, 112, 1),
    )


def field_kernel(counts, orb, prev, comp, mate, ext, *refs):
    sends, mate32, pos = list(refs[:-1]), refs[-1], position(counts)
    mate32[...] = mate[: mate32.shape[0], :].astype(F32)
    bx, bands, row_lanes = orb.shape
    half = bands // 2
    fx, fy = prev.shape[0] * LANES // (2 * BY * 2 * BZ), 2 * BY
    groups = prev.shape[0] // 3
    lane = lane_iota(groups)
    own = (lane >= ZOFF) & (lane < ZOFF + 2 * BZ)
    first = pos[2] == 0
    shift = jnp.where(first, 2 * BZ, LANES - 2 * BZ)
    edge_low = jnp.where(first, ZOFF + 2 * BZ, 0)
    edge_high = jnp.where(first, LANES, ZOFF)
    edge = (lane >= edge_low) & (lane < edge_high)
    rows = fx * fy
    for f, ref in enumerate((prev, comp)):
        mine = field_rows(ref, groups)
        theirs = field_rows(mate32.at[pl.ds(f * prev.shape[0], prev.shape[0])], groups)
        for k in range(4):
            halo = jnp.where(edge, pltpu.roll(theirs[k], shift, 1), 0.0)
            ext[pl.ds(f * rows + k, groups, stride=4), :] = jnp.where(own, mine[k], halo)
    widths = (WV, WS)
    x_sides, y_sides = sides(counts[0]), sides(counts[1])
    for side in x_sides:
        send, done = sends.pop(0), 0
        for f, width in enumerate(widths):
            start = f * rows + fy * rim_start(side, pos[0], fx, width)
            send[pl.ds(done, width * fy), :] = ext[pl.ds(pl.multiple_of(start, 8), width * fy), :].astype(BF16)
            done += width * fy
    first_half = lane_iota(half) < BZ
    for side in y_sides:
        send = sends.pop(0)
        start = pl.multiple_of(rim_start(side, pos[1], row_lanes, LANES), LANES)
        turn = jnp.where(pos[1] == 0, BZ, 0) if side == "swap" else (BZ if side == "lo" else 0)
        for x in range(bx):
            face = orb[x, :, pl.ds(start, LANES)].astype(F32)
            both = jnp.where(first_half, pltpu.roll(face[:half], turn, 1), pltpu.roll(face[half:], turn + BZ, 1))
            send[pl.ds(x * half, half), :] = both.astype(BF16)
        at = rim_start(side, pos[1], fy, PAD)
        for f in range(2):
            cut = [ext[pl.ds(pl.multiple_of(f * rows + fy * x + at, 8), PAD), :] for x in range(fx)]
            send[pl.ds(bx * half + f * fx * PAD, fx * PAD), :] = jnp.concatenate(cut, 0).astype(BF16)
    for x_side in x_sides:
        for y_side in y_sides:
            send = sends.pop(0)
            at = rim_start(y_side, pos[1], fy, PAD)
            cut = []
            for f, width in enumerate(widths):
                start = rim_start(x_side, pos[0], fx, width)
                cut += [
                    ext[pl.ds(pl.multiple_of(f * rows + fy * (start + x) + at, 8), PAD), :]
                    for x in range(width)
                ]
            cut.append(jnp.zeros((PAD, LANES), F32))
            send[...] = jnp.concatenate(cut, 0).astype(BF16)


def merge_rows(flat, joined):
    per = 384 // BZ
    groups = flat.shape[0] // per
    lane = lane_iota(groups)
    r = [pltpu.roll(flat[pl.ds(k, groups, stride=per), :], BZ * k % LANES, 1) for k in range(per)]
    for j in range(3):
        tile = None
        for k in range(per):
            low, high = BZ * k - LANES * j, BZ * (k + 1) - LANES * j
            if high > 0 and low < LANES:
                tile = r[k] if tile is None else jnp.where(lane >= low, r[k], tile)
        joined[pl.ds(j, groups, stride=3), :] = tile
    tiles = BY * BZ // LANES
    planes = flat.shape[0] // BY
    columns = [joined[pl.ds(t, planes, stride=tiles), :] for t in range(tiles)]
    rows = jnp.concatenate(columns, 1)
    return [rows[x : x + 1] for x in range(planes)]


def local_kernel(counts, chip, local_potential, out, flat, joined):
    cz = position(counts)[2]
    rho = (3.0 / math.pi) * pltpu.roll(chip[...], jnp.where(cz == 0, 0, LANES - BZ), 1)
    safe = jnp.where(rho > 0.0, rho, 1.0)
    root = jnp.exp(jnp.log(safe) * (1.0 / 3.0))
    root = root - (root - safe / (root * root)) * (1.0 / 3.0)
    flat[...] = jnp.where(rho > 0.0, root, 0.0)
    for x, row in enumerate(merge_rows(flat, joined)):
        out[x : x + 1, :] = local_potential[x] - row


def finish_kernel(counts, *refs):
    it = iter(refs)
    chip, ext, local_part, orb, inner, mate_block = (next(it) for _ in range(6))
    x_sides, y_sides = sides(counts[0]), sides(counts[1])
    xy_sides = [(a, b) for a in x_sides for b in y_sides]
    rho_x, rho_y, rho_xy = ([next(it) for _ in s] for s in (x_sides, y_sides, xy_sides))
    fld_x, fld_y = ([next(it) for _ in s] for s in (x_sides, y_sides))
    x_faces = [next(it) for _ in x_sides]
    out, potential_out = next(it), next(it)
    coarse, wide, fine, v0, v1, src, flat, effective, potential, result, store, store_potential = it
    cx, cy, cz = position(counts)
    bands = orb.shape[1]
    bx = chip.shape[0] // BY
    fx, fy = 2 * bx, 2 * BY
    ry, rc = fy + 2 * PAD, BY + 2 * PAD
    qx = fx + 2 * WV
    face_rows = bx * bands // 2

    coarse[...] = jnp.zeros_like(coarse)
    for x in range(bx):
        coarse[WC + x, PAD : PAD + BY, :] = chip[x * BY : (x + 1) * BY, :]
    for side, ref in zip(x_sides, rho_x):
        at = halo_start(side, cx, 0, WC + bx)
        block = ref[...].astype(F32)
        for x in range(WC):
            coarse[at + x, PAD : PAD + BY, :] = block[x * BY : (x + 1) * BY, :]
    for side, ref in zip(y_sides, rho_y):
        at = pl.multiple_of(halo_start(side, cy, 0, PAD + BY), 8)
        block = ref[...].astype(F32)
        for x in range(bx):
            coarse[WC + x, pl.ds(at, PAD), :] = block[x * PAD : (x + 1) * PAD, :]
    for (x_side, y_side), ref in zip(xy_sides, rho_xy):
        at_x = halo_start(x_side, cx, 0, WC + bx)
        at = pl.multiple_of(halo_start(y_side, cy, 0, PAD + BY), 8)
        block = ref[...].astype(F32)
        for x in range(WC):
            coarse[at_x + x, pl.ds(at, PAD), :] = block[x * PAD : (x + 1) * PAD, :]

    v0[...] = jnp.zeros_like(v0)
    v1[:, 0:PAD, :] = jnp.zeros((qx, PAD, LANES), F32)
    v1[:, ry - PAD : ry, :] = jnp.zeros((qx, PAD, LANES), F32)
    src[...] = jnp.zeros_like(src)
    for f, (ref, width) in enumerate(((v0, WV), (src, WS))):
        rows = f * fx * fy
        for x in range(fx):
            ref[WV + x, PAD : PAD + fy, :] = ext[rows + x * fy : rows + (x + 1) * fy, :]
        done = f * WV
        for side, got in zip(x_sides, fld_x):
            at = halo_start(side, cx, WV - width, WV + fx)
            for x in range(width):
                ref[at + x, PAD : PAD + fy, :] = got[(done + x) * fy : (done + x + 1) * fy, :].astype(F32)
        for side, got in zip(y_sides, fld_y):
            at = pl.multiple_of(halo_start(side, cy, 0, PAD + fy), 8)
            block = got[face_rows + f * fx * PAD : face_rows + (f + 1) * fx * PAD, :].astype(F32)
            for x in range(fx):
                ref[WV + x, pl.ds(at, PAD), :] = block[x * PAD : (x + 1) * PAD, :]
        for (x_side, y_side), got in zip(xy_sides, rho_xy):
            at_x = halo_start(x_side, cx, WV - width, WV + fx)
            at = pl.multiple_of(halo_start(y_side, cy, 0, PAD + fy), 8)
            block = got[(WC + 1) * PAD :, :].astype(F32)
            for x in range(width):
                ref[at_x + x, pl.ds(at, PAD), :] = block[(done + x) * PAD : (done + x + 1) * PAD, :]

    cells = (bx + 2 * WC) * rc
    wide[...] = wide_dot(coarse[...].reshape(cells, LANES), z_refine(cz))
    for p in range(bx + 2 * WC):
        base, half = p * rc + PAD // 2, ry // 2
        here = 0.75 * wide[pl.ds(base, half), :]
        fine[pl.ds(p * ry, half, stride=2), :] = here + 0.25 * wide[pl.ds(base - 1, half), :]
        fine[pl.ds(p * ry + 1, half, stride=2), :] = here + 0.25 * wide[pl.ds(base + 1, half), :]
    for q in range(1, qx - 1):
        at = q - WV
        here, other = at // 2 + WC, at // 2 + WC + (1 if at % 2 else -1)
        refined = 0.75 * fine[pl.ds(here * ry, ry), :] + 0.25 * fine[pl.ds(other * ry, ry), :]
        src[q] = math.pi * (refined - src[q])

    near, span = PAD - WS, fy + 2 * WS
    row = lax.broadcasted_iota(jnp.int32, (span, LANES), 0) - WS + fy * cy
    lane = lane_iota(span) - ZOFF + 2 * BZ * cz
    inside = (row >= 0) & (row < fy * counts[1]) & (lane >= 0) & (lane < 2 * BZ * counts[2])
    share = jnp.where(inside, 1.0 / 6.0, 0.0)
    old, new = v0, v1
    beside = z_neighbours()
    for sweep in range(SWEEPS):
        first, last = sweep + 1, qx - sweep - 1
        rows = old[first:last, near : near + span, :].reshape((last - first) * span, LANES)
        along_z = wide_dot(rows, beside)
        for q in range(first, last):
            at = q - WV + fx * cx
            total = along_z[(q - first) * span : (q - first + 1) * span]
            total = total + old[q - 1, near : near + span, :] + old[q + 1, near : near + span, :]
            total = total + old[q, near - 1 : near - 1 + span, :] + old[q, near + 1 : near + 1 + span, :]
            total = (total + src[q, near : near + span, :]) * share
            if q < WV or q >= WV + fx:
                total = jnp.where((at >= 0) & (at < fx * counts[0]), total, 0.0)
            new[q, near : near + span, :] = total
        old, new = new, old

    groups = fy // 4
    lane = lane_iota(groups)
    for x in range(fx):
        r = [old[WV + x, pl.ds(PAD + k, groups, stride=4), :] for k in range(4)]
        r1, r2 = pltpu.roll(r[1], 80, 1), pltpu.roll(r[2], 48, 1)
        potential[pl.ds(3 * groups * x, groups, stride=3), :] = jnp.where(lane < 96, pltpu.roll(r[0], 112, 1), r1)
        potential[pl.ds(3 * groups * x + 1, groups, stride=3), :] = jnp.where(lane < 64, r1, r2)
        potential[pl.ds(3 * groups * x + 2, groups, stride=3), :] = jnp.where(lane < 32, r2, pltpu.roll(r[3], 16, 1))

    send_potential = pltpu.make_async_copy(potential, potential_out, store_potential)
    send_potential.start()

    pieces = []
    for x in range(bx):
        q = WV + 2 * x
        fine[pl.ds(x * ry, ry), :] = 0.125 * (old[q - 1] + old[q + 2]) + 0.375 * (old[q] + old[q + 1])
        rows = [fine[pl.ds(x * ry + PAD + k, BY, stride=2), :] for k in (-1, 0, 1, 2)]
        pieces.append(0.125 * (rows[0] + rows[3]) + 0.375 * (rows[1] + rows[2]))
    back = wide_dot(jnp.concatenate(pieces, 0), z_coarsen())
    flat[...] = back
    for x, row in enumerate(merge_rows(flat, wide)):
        effective[x : x + 1, :] = row + local_part[x : x + 1, :]

    width, half = effective.shape[1], bands // 2
    lane = lane_iota(half)
    lane = jnp.concatenate([lane, lane], 0)
    spread = z_spread(cz)
    z_faces = mate_block[2 * potential.shape[0] :, :]
    step = 2 * LANES
    stores = []
    for j in range(0, width, step):
        columns = min(step, width - j)
        outer = jnp.dot(z_faces, spread[:, j : j + columns], preferred_element_type=F32)
        for x in range(bx):
            for t in range(j, j + columns, LANES):
                cut = slice(t, t + LANES)
                total = inner[x, :, cut] + effective[x : x + 1, cut] * orb[x, :, cut].astype(F32)
                total = total + outer[x * bands : (x + 1) * bands, t - j : t - j + LANES]
                for side, face in zip(y_sides, fld_y):
                    halo = -0.5 * face[x * half : (x + 1) * half, :].astype(F32)
                    if t == 0 and side != "hi":
                        here = jnp.concatenate([halo, pltpu.roll(halo, LANES - BZ, 1)], 0)
                        total = total + jnp.where((lane < BZ) & (cy > 0), here, 0.0)
                    if t == width - LANES and side != "lo":
                        here = [pltpu.roll(halo, LANES - BZ, 1), pltpu.roll(halo, LANES - 2 * BZ, 1)]
                        keep = (lane >= LANES - BZ) & (cy < counts[1] - 1)
                        total = total + jnp.where(keep, jnp.concatenate(here, 0), 0.0)
                for side, face in zip(x_sides, x_faces):
                    if x == 0 and side != "hi":
                        total = total + jnp.where(cx > 0, -0.5, 0.0) * face[:, cut].astype(F32)
                    if x == bx - 1 and side != "lo":
                        total = total + jnp.where(cx < counts[0] - 1, -0.5, 0.0) * face[:, cut].astype(F32)
                result[x, :, cut] = total.astype(BF16)
        cut = pl.ds(j, columns)
        stores.append(pltpu.make_async_copy(result.at[:, :, cut], out.at[:, :, cut], store.at[j // step]))
        stores[-1].start()
    for copy in stores + [send_potential]:
        copy.wait()


def laplace_kernel(orb, out):
    planes, bands, width = orb.shape
    step = 2 * LANES
    weights = [stencil(step * p % BZ, step) for p in range(3)]
    for j in range(0, width, step):
        columns = min(step, width - j)
        first, last = max(j - LANES, 0), min(j + step + LANES, width)
        skip = first - (j - LANES)
        w = weights[j // step % 3][skip : skip + last - first, :columns]
        here = orb[:, :, first:last].reshape(planes * bands, last - first)
        total = jnp.dot(here, w, preferred_element_type=F32).reshape(planes, bands, columns)
        for x in range(planes):
            near = [orb[n, :, j : j + columns].astype(F32) for n in (x - 1, x + 1) if 0 <= n < planes]
            out[x, :, j : j + columns] = total[x] - 0.5 * sum(near)


def vmem():
    return pl.BlockSpec(memory_space=pltpu.VMEM)


def local(mesh, orbitals, occupations, previous, compensation, local_potential):
    return step(mesh, orbitals, occupations, previous, compensation, local_potential)


def step(mesh, orbitals, occupations, previous, compensation, local_potential):
    domains, groups = mesh.shape["dom"], mesh.shape["band"]
    split_z = 2
    split_y = min(4, domains // 4)
    counts = (domains // (split_y * split_z), split_y, split_z)
    bands, _, bx, width = orbitals.shape
    tiles = width // LANES
    fx, fy = 2 * bx, 2 * BY
    x_sides, y_sides = sides(counts[0]), sides(counts[1])
    xy_sides = [(a, b) for a in x_sides for b in y_sides]
    moves = [{0: s} for s in x_sides] + [{1: s} for s in y_sides] + [{0: a, 1: b} for a, b in xy_sides]
    hbm = pl.BlockSpec(memory_space=pltpu.HBM)

    def shape(*dims, dtype=F32):
        return jax.ShapeDtypeStruct(dims, dtype)

    def params(kib):
        return pltpu.CompilerParams(vmem_limit_bytes=kib * 2**10)

    flat = [a.reshape(fx * fy * 2 * BZ // LANES, LANES) for a in (previous, compensation)]
    orb = jnp.transpose(orbitals.reshape(bands, bx, width), (1, 0, 2))
    mate_rows = 2 * flat[0].shape[0] + bx * bands
    inputs = [orb, occupations.reshape(1, bands), *flat]
    part, orb, mate_block, *x_faces = pl.pallas_call(
        functools.partial(density_kernel, counts),
        in_specs=[hbm] * 4,
        out_specs=[vmem()] * (3 + len(x_sides)),
        out_shape=[shape(bx * tiles, LANES), shape(*orb.shape, dtype=BF16)]
        + [shape(mate_rows, LANES, dtype=BF16)]
        + [shape(bands, width, dtype=BF16) for _ in x_sides],
        scratch_shapes=[
            pltpu.VMEM((1, bands), F32),
            pltpu.VMEM((2, *flat[0].shape), F32),
            pltpu.SemaphoreType.DMA((bx,)),
            pltpu.SemaphoreType.DMA(()),
            pltpu.SemaphoreType.DMA((2,)),
        ],
        compiler_params=params(8 * 1024),
        name="density",
    )(*(pltpu.with_memory_space_constraint(a, pltpu.HBM) for a in inputs))
    x_faces = [fetch(f, counts, {0: s}) for s, f in zip(x_sides, x_faces)]
    mate_block = fetch(mate_block, counts, {2: "swap"})
    parts = [part]
    for shift in range(1, groups):
        route = [(i, i ^ shift if groups & (groups - 1) == 0 else (i + shift) % groups) for i in range(groups)]
        parts.append(lax.ppermute(part, "band", route))

    inner = pl.pallas_call(
        laplace_kernel,
        in_specs=[vmem()],
        out_specs=vmem(),
        out_shape=shape(bx, bands, width),
        compiler_params=params(16 * 1024),
        cost_estimate=pl.CostEstimate(flops=6 * 10**9, bytes_accessed=8 * 10**6, transcendentals=0),
        name="laplace",
    )(orb)

    rim_rows = [(WV + WS) * fy] * len(x_sides) + [bx * bands // 2 + 2 * fx * PAD] * len(y_sides)
    rim_rows += [(WV + WS + 1) * PAD] * len(xy_sides)
    ext, *rims = pl.pallas_call(
        functools.partial(field_kernel, counts),
        in_specs=[vmem()] * 4,
        out_specs=[vmem()] * (1 + len(rim_rows)),
        out_shape=[shape(2 * fx * fy, LANES)] + [shape(n, LANES, dtype=BF16) for n in rim_rows],
        scratch_shapes=[pltpu.VMEM((2 * flat[0].shape[0], LANES), F32)],
        compiler_params=params(4 * 1024),
        cost_estimate=pl.CostEstimate(flops=3 * 10**9, bytes_accessed=10**6, transcendentals=0),
        name="fields",
    )(orb, *flat, mate_block)
    corner_rims = rims[len(x_sides) + len(y_sides) :]
    fields = [fetch(r, counts, m) for r, m in zip(rims, moves) if list(m) == [0]]
    fields += [fetch(r, counts, m) for r, m in zip(rims, moves) if list(m) == [1]]

    rho = pl.pallas_call(
        functools.partial(total_kernel, counts, 1.0 / (bands * groups)),
        in_specs=[vmem()] * groups,
        out_specs=vmem(),
        out_shape=shape(bx * BY, LANES),
        scratch_shapes=[pltpu.VMEM((bx * tiles, LANES), F32)],
        compiler_params=params(1024),
        name="total",
    )(*parts)
    mate = fetch(rho, counts, {2: "swap"})
    corner_rows = (WC + 1) * PAD + (WV + WS + 1) * PAD
    cut_rows = [WC * BY] * len(x_sides) + [bx * PAD] * len(y_sides) + [corner_rows] * len(xy_sides)
    chip, *cuts = pl.pallas_call(
        functools.partial(cut_kernel, counts),
        in_specs=[vmem()] * (2 + len(corner_rims)),
        out_specs=[vmem()] * (1 + len(cut_rows)),
        out_shape=[shape(bx * BY, LANES)] + [shape(n, LANES, dtype=BF16) for n in cut_rows],
        compiler_params=params(1024),
        name="cut",
    )(rho, mate, *corner_rims)
    densities = [fetch(c, counts, m) for c, m in zip(cuts, moves)]

    rc, ry, qx = BY + 2 * PAD, fy + 2 * PAD, fx + 2 * WV
    local_rows = jnp.transpose(local_potential, (1, 0, 2))
    local_part = pl.pallas_call(
        functools.partial(local_kernel, counts),
        in_specs=[vmem(), vmem()],
        out_specs=vmem(),
        out_shape=shape(bx, width),
        scratch_shapes=[pltpu.VMEM((bx * BY, LANES), F32), pltpu.VMEM((bx * tiles, LANES), F32)],
        compiler_params=params(1024),
        name="local",
    )(chip, local_rows)
    operands = [chip, ext, local_part, orb, inner, mate_block, *densities, *fields, *x_faces]
    applied, potential = pl.pallas_call(
        functools.partial(finish_kernel, counts),
        in_specs=[vmem()] * len(operands),
        out_specs=[hbm, hbm],
        scratch_shapes=[
            pltpu.VMEM((bx + 2 * WC, rc, LANES), F32),
            pltpu.VMEM(((bx + 2 * WC) * rc, LANES), F32),
            pltpu.VMEM(((bx + 2 * WC) * ry, LANES), F32),
            pltpu.VMEM((qx, ry, LANES), F32),
            pltpu.VMEM((qx, ry, LANES), F32),
            pltpu.VMEM((qx, ry, LANES), F32),
            pltpu.VMEM((bx * BY, LANES), F32),
            pltpu.VMEM((bx, width), F32),
            pltpu.VMEM(flat[0].shape, F32),
            pltpu.VMEM((bx, bands, width), BF16),
            pltpu.SemaphoreType.DMA((pl.cdiv(width, 2 * LANES),)),
            pltpu.SemaphoreType.DMA(()),
        ],
        out_shape=[shape(bx, bands, width, dtype=BF16), shape(*flat[0].shape)],
        compiler_params=params(20 * 1024),
        name="finish",
    )(*operands)
    applied = jnp.transpose(applied, (1, 0, 2)).reshape(orbitals.shape)
    return applied, potential.reshape(previous.shape)


def solution(mesh):
    return jax.shard_map(
        functools.partial(local, mesh),
        mesh=mesh,
        in_specs=(
            P("band", "dom", None, None),
            P("band"),
            P("dom", None, None),
            P("dom", None, None),
            P("dom", None, None),
        ),
        out_specs=(P("band", "dom", None, None), P("dom", None, None)),
        check_vma=False,
    )
```

```python
import functools
import math

import jax
import jax.numpy as jnp
import numpy as np
from jax import lax
from jax.experimental import pallas as pl
from jax.experimental.pallas import tpu as pltpu
from jax.sharding import PartitionSpec as P


BY = 24
BZ = 48
SWEEPS = 4

F32, BF16 = jnp.float32, jnp.bfloat16
LANES = 128
PAD = 8
ZOFF = 16
WV = SWEEPS + 1
WS = SWEEPS
WC = WS // 2 + 1


def sides(count):
    return ("swap",) if count == 2 else ("lo", "hi")


def fetch(block, counts, moves):
    pairs = []
    for target in np.ndindex(*counts):
        source = list(target)
        for axis, side in moves.items():
            source[axis] = {"swap": 1 - target[axis], "lo": target[axis] - 1, "hi": target[axis] + 1}[side]
        if all(0 <= s < n for s, n in zip(source, counts)):
            pairs.append((int(np.ravel_multi_index(source, counts)), int(np.ravel_multi_index(target, counts))))
    return lax.ppermute(block, "dom", pairs)


def rim_start(side, coord, length, width):
    if side == "swap":
        return jnp.where(coord == 0, length - width, 0)
    return length - width if side == "lo" else 0


def halo_start(side, coord, low, high):
    if side == "swap":
        return jnp.where(coord == 0, high, low)
    return low if side == "lo" else high


def position(counts):
    at = lax.axis_index("dom")
    return at // (counts[1] * counts[2]), at // counts[2] % counts[1], at % counts[2]


def lane_iota(rows):
    return lax.broadcasted_iota(jnp.int32, (rows, LANES), 1)


def halves(value):
    high = value.astype(BF16)
    return jnp.concatenate([high, (value - high.astype(F32)).astype(BF16)], 1)


def wide_dot(value, weights):
    return jnp.dot(halves(value), jnp.concatenate([weights, weights], 0), preferred_element_type=F32)


def grid2(rows, columns):
    shape = (rows, columns)
    return (lax.broadcasted_iota(jnp.int32, shape, d) for d in (0, 1))


def z_refine(core):
    cell, lane = grid2(LANES, LANES)
    fine = lane - ZOFF + 2 * BZ * core
    here = fine >> 1
    other = here + 2 * (fine & 1) - 1
    return jnp.where(cell == here, 0.75, jnp.where(cell == other, 0.25, 0.0)).astype(BF16)


def z_coarsen():
    lane, cell = grid2(LANES, LANES)
    step = lane - ZOFF - 2 * cell
    w = jnp.where((step == 0) | (step == 1), 0.375, jnp.where((step == -1) | (step == 2), 0.125, 0.0))
    return jnp.where(cell < BZ, w, 0.0).astype(BF16)


def z_neighbours():
    source, lane = grid2(LANES, LANES)
    step = source - lane
    return jnp.where((step == 1) | (step == -1), 1.0, 0.0).astype(BF16)


def z_columns(core, rows):
    lane = lane_iota(rows)
    at = BZ * (lane % BY) + jnp.where(core == 0, BZ - 1 - lane // BY, lane // BY)
    return jnp.where(lane < WC * BY, at, -1)


def z_pick(core, lanes):
    lane, _ = grid2(lanes, LANES)
    return jnp.where(lane == z_columns(core, 1), 1.0, 0.0).astype(BF16)


def z_place(core):
    column, lane = grid2(LANES, LANES)
    z = jnp.where(core == 0, BZ + column // BY, BZ - 1 - column // BY)
    return jnp.where((lane == z) & (column < WC * BY), 1.0, 0.0).astype(BF16)


def z_spread(core):
    y, lane = grid2(LANES, BY * BZ)
    return jnp.where(lane == BZ * y + jnp.where(core == 0, BZ - 1, 0), -0.5, 0.0).astype(BF16)


def lanes_of(value, index):
    pieces = [value[r : r + 8] for r in range(0, value.shape[0], 8)]
    return [jnp.take_along_axis(p, index, axis=1, mode="promise_in_bounds") for p in pieces]


def stencil(first, columns):
    source, lane = grid2(4 * LANES, columns)
    step = source - LANES - lane
    z = (lax.broadcasted_iota(jnp.int32, (1, columns), 1) + first) % BZ
    up = jnp.where(z == BZ - 1, 2 * BY * BZ, 1)
    down = jnp.where(z == 0, 2 * BY * BZ, -1)
    near = (step == up) | (step == down) | (step == BZ) | (step == -BZ)
    return jnp.where(near, -0.5, jnp.where(step == 0, 3.0, 0.0)).astype(BF16)


def sum_rows(value):
    while value.shape[0] % 16 == 0:
        half = value.shape[0] // 2
        value = value[:half] + value[half:]
    return jnp.sum(value, axis=0, keepdims=True)


def density_kernel(counts, orb, occ, prev, comp, part, held, mate_sent, weight_out, *refs):
    x_faces, (weights, fields, load, load_occ, load_field) = refs[:-5], refs[-5:]
    planes, bands, width = held.shape
    tiles, rows = width // LANES, prev.shape[0]
    pos = position(counts)
    first = pltpu.make_async_copy(occ, weights, load_occ)
    first.start()
    loads = [pltpu.make_async_copy(orb.at[x], held.at[x], load.at[x]) for x in range(planes)]
    loads += [pltpu.make_async_copy(ref, fields.at[f], load_field.at[f]) for f, ref in enumerate((prev, comp))]
    for copy in loads:
        copy.start()
    split = min(4, tiles)
    pick = z_pick(pos[2], split * LANES)
    face_lane = z_columns(pos[2], 8)
    first.wait()
    column = jnp.broadcast_to(weights[...], (LANES, bands))
    column = jnp.concatenate([column, jnp.zeros((LANES, -bands % LANES), F32)], 1)
    weight = jnp.concatenate([column[:, b : b + LANES].T for b in range(0, bands, LANES)], 0)[:bands]
    weight_out[...] = weight
    for x in range(planes):
        loads[x].wait()
        face = jnp.dot(held[x, :, : split * LANES], pick, preferred_element_type=F32)
        for t in range(tiles):
            f = held[x, :, t * LANES : (t + 1) * LANES].astype(F32)
            part[tiles * x + t : tiles * x + t + 1, :] = sum_rows(f * f * weight)
            if t >= split:
                at = face_lane - t * LANES
                got = lanes_of(f, at & (LANES - 1))
                face = [jnp.where(at >= 0, new, face[8 * i : 8 * i + 8]) for i, new in enumerate(got)]
                face = jnp.concatenate(face, 0)
        mate_sent[2 * rows + x * bands : 2 * rows + (x + 1) * bands, :] = face.astype(BF16)
    for side, face in zip(sides(counts[0]), x_faces):
        face[...] = held[rim_start(side, pos[0], planes, 1)]
    for f in range(2):
        loads[planes + f].wait()
        mate_sent[f * rows : (f + 1) * rows, :] = fields[f].astype(BF16)


def strip_kernel(part, mate, weight, out):
    rows, bands = part.shape[0], weight.shape[0]
    out[:rows, :] = part[...]
    for x in range(out.shape[0] - rows):
        start = mate.shape[0] - (out.shape[0] - rows - x) * bands
        f = mate[start : start + bands, :].astype(F32)
        out[rows + x : rows + x + 1, :] = sum_rows(f * f * weight[...])


def total_kernel(counts, scale, bands_parts, *refs):
    parts, refs = refs[:bands_parts], refs[bands_parts:]
    x_sides, y_sides = sides(counts[0]), sides(counts[1])
    corners = len(x_sides) * len(y_sides)
    fields, chip, sends, flat = list(refs[:corners]), refs[corners], list(refs[corners + 1 : -1]), refs[-1]
    cx, cy, cz = position(counts)
    total = parts[0][...]
    for part in parts[1:]:
        total = total + part[...]
    flat[...] = total * scale
    per = 384 // BZ
    bx = chip.shape[0] // BY
    groups = chip.shape[0] // per
    lane = lane_iota(groups)
    shift = jnp.where(cz == 0, 0, BZ)
    tile = [flat[pl.ds(j, groups, stride=3), :] for j in range(3)]
    for k in range(per):
        at, off = divmod(BZ * k, LANES)
        row = pltpu.roll(tile[at], (LANES - off) % LANES, 1) if off else tile[at]
        if off + BZ > LANES:
            row = jnp.where(lane < LANES - off, row, pltpu.roll(tile[at + 1], LANES - off, 1))
        row = jnp.where(lane < BZ, row, 0.0)
        chip[pl.ds(k, groups, stride=per), :] = pltpu.roll(row, shift, 1)
    y, column = grid2(BY, LANES)
    mine = column % BY == y
    strips = [jnp.where(mine, flat[3 * groups + x : 3 * groups + x + 1, :], 0.0) for x in range(bx)]
    chip[...] = chip[...] + wide_dot(jnp.concatenate(strips, 0), z_place(cz))
    for side in x_sides:
        at = pl.multiple_of(BY * rim_start(side, cx, bx, WC), 8)
        sends.pop(0)[...] = chip[pl.ds(at, WC * BY), :].astype(BF16)
    for side in y_sides:
        at = rim_start(side, cy, BY, PAD)
        rows = [chip[pl.ds(pl.multiple_of(BY * x + at, 8), PAD), :] for x in range(bx)]
        sends.pop(0)[...] = jnp.concatenate(rows, 0).astype(BF16)
    for x_side in x_sides:
        for y_side in y_sides:
            at_x, at = rim_start(x_side, cx, bx, WC), rim_start(y_side, cy, BY, PAD)
            rows = [chip[pl.ds(pl.multiple_of(BY * (at_x + x) + at, 8), PAD), :] for x in range(WC)]
            rows.append(jnp.zeros((PAD, LANES), F32))
            rows = jnp.concatenate(rows, 0).astype(BF16)
            sends.pop(0)[...] = jnp.concatenate([rows, fields.pop(0)[...]], 0)


def field_rows(ref, groups):
    lane = lane_iota(groups)
    a, b, c = (ref[pl.ds(j, groups, stride=3), :] for j in range(3))
    return (
        pltpu.roll(a, 16, 1),
        jnp.where(lane < 48, pltpu.roll(a, 48, 1), pltpu.roll(b, 48, 1)),
        jnp.where(lane < 80, pltpu.roll(b, 80, 1), pltpu.roll(c, 80, 1)),
        pltpu.roll(c, 112, 1),
    )


def field_kernel(counts, orb, prev, comp, mate, ext, *refs):
    sends, mate32, pos = list(refs[:-1]), refs[-1], position(counts)
    mate32[...] = mate[: mate32.shape[0], :].astype(F32)
    bx, bands, row_lanes = orb.shape
    half = bands // 2
    fx, fy = prev.shape[0] * LANES // (2 * BY * 2 * BZ), 2 * BY
    groups = prev.shape[0] // 3
    lane = lane_iota(groups)
    own = (lane >= ZOFF) & (lane < ZOFF + 2 * BZ)
    first = pos[2] == 0
    shift = jnp.where(first, 2 * BZ, LANES - 2 * BZ)
    edge_low = jnp.where(first, ZOFF + 2 * BZ, 0)
    edge_high = jnp.where(first, LANES, ZOFF)
    edge = (lane >= edge_low) & (lane < edge_high)
    rows = fx * fy
    for f, ref in enumerate((prev, comp)):
        mine = field_rows(ref, groups)
        theirs = field_rows(mate32.at[pl.ds(f * prev.shape[0], prev.shape[0])], groups)
        for k in range(4):
            halo = jnp.where(edge, pltpu.roll(theirs[k], shift, 1), 0.0)
            ext[pl.ds(f * rows + k, groups, stride=4), :] = jnp.where(own, mine[k], halo)
    widths = (WV, WS)
    x_sides, y_sides = sides(counts[0]), sides(counts[1])
    for side in x_sides:
        send, done = sends.pop(0), 0
        for f, width in enumerate(widths):
            start = f * rows + fy * rim_start(side, pos[0], fx, width)
            send[pl.ds(done, width * fy), :] = ext[pl.ds(pl.multiple_of(start, 8), width * fy), :].astype(BF16)
            done += width * fy
    first_half = lane_iota(half) < BZ
    for side in y_sides:
        send = sends.pop(0)
        start = pl.multiple_of(rim_start(side, pos[1], row_lanes, LANES), LANES)
        turn = jnp.where(pos[1] == 0, BZ, 0) if side == "swap" else (BZ if side == "lo" else 0)
        for x in range(bx):
            face = orb[x, :, pl.ds(start, LANES)].astype(F32)
            both = jnp.where(first_half, pltpu.roll(face[:half], turn, 1), pltpu.roll(face[half:], turn + BZ, 1))
            send[pl.ds(x * half, half), :] = both.astype(BF16)
        at = rim_start(side, pos[1], fy, PAD)
        for f in range(2):
            cut = [ext[pl.ds(pl.multiple_of(f * rows + fy * x + at, 8), PAD), :] for x in range(fx)]
            send[pl.ds(bx * half + f * fx * PAD, fx * PAD), :] = jnp.concatenate(cut, 0).astype(BF16)
    for x_side in x_sides:
        for y_side in y_sides:
            send = sends.pop(0)
            at = rim_start(y_side, pos[1], fy, PAD)
            cut = []
            for f, width in enumerate(widths):
                start = rim_start(x_side, pos[0], fx, width)
                cut += [
                    ext[pl.ds(pl.multiple_of(f * rows + fy * (start + x) + at, 8), PAD), :]
                    for x in range(width)
                ]
            cut.append(jnp.zeros((PAD, LANES), F32))
            send[...] = jnp.concatenate(cut, 0).astype(BF16)


def merge_rows(flat, joined):
    per = 384 // BZ
    groups = flat.shape[0] // per
    lane = lane_iota(groups)
    r = [pltpu.roll(flat[pl.ds(k, groups, stride=per), :], BZ * k % LANES, 1) for k in range(per)]
    for j in range(3):
        tile = None
        for k in range(per):
            low, high = BZ * k - LANES * j, BZ * (k + 1) - LANES * j
            if high > 0 and low < LANES:
                tile = r[k] if tile is None else jnp.where(lane >= low, r[k], tile)
        joined[pl.ds(j, groups, stride=3), :] = tile
    tiles = BY * BZ // LANES
    planes = flat.shape[0] // BY
    columns = [joined[pl.ds(t, planes, stride=tiles), :] for t in range(tiles)]
    rows = jnp.concatenate(columns, 1)
    return [rows[x : x + 1] for x in range(planes)]


def local_kernel(counts, chip, local_potential, out, flat, joined):
    cz = position(counts)[2]
    rho = (3.0 / math.pi) * pltpu.roll(chip[...], jnp.where(cz == 0, 0, LANES - BZ), 1)
    safe = jnp.where(rho > 0.0, rho, 1.0)
    root = jnp.exp(jnp.log(safe) * (1.0 / 3.0))
    root = root - (root - safe / (root * root)) * (1.0 / 3.0)
    flat[...] = jnp.where(rho > 0.0, root, 0.0)
    for x, row in enumerate(merge_rows(flat, joined)):
        out[x : x + 1, :] = local_potential[x] - row


def finish_kernel(counts, *refs):
    it = iter(refs)
    chip, ext, local_part, orb, inner, mate_block = (next(it) for _ in range(6))
    x_sides, y_sides = sides(counts[0]), sides(counts[1])
    xy_sides = [(a, b) for a in x_sides for b in y_sides]
    rho_x, rho_y, rho_xy = ([next(it) for _ in s] for s in (x_sides, y_sides, xy_sides))
    fld_x, fld_y = ([next(it) for _ in s] for s in (x_sides, y_sides))
    x_faces = [next(it) for _ in x_sides]
    out, potential_out = next(it), next(it)
    coarse, wide, fine, v0, v1, src, flat, effective, potential, result, store, store_potential = it
    cx, cy, cz = position(counts)
    bands = orb.shape[1]
    bx = chip.shape[0] // BY
    fx, fy = 2 * bx, 2 * BY
    ry, rc = fy + 2 * PAD, BY + 2 * PAD
    qx = fx + 2 * WV
    face_rows = bx * bands // 2

    coarse[...] = jnp.zeros_like(coarse)
    for x in range(bx):
        coarse[WC + x, PAD : PAD + BY, :] = chip[x * BY : (x + 1) * BY, :]
    for side, ref in zip(x_sides, rho_x):
        at = halo_start(side, cx, 0, WC + bx)
        block = ref[...].astype(F32)
        for x in range(WC):
            coarse[at + x, PAD : PAD + BY, :] = block[x * BY : (x + 1) * BY, :]
    for side, ref in zip(y_sides, rho_y):
        at = pl.multiple_of(halo_start(side, cy, 0, PAD + BY), 8)
        block = ref[...].astype(F32)
        for x in range(bx):
            coarse[WC + x, pl.ds(at, PAD), :] = block[x * PAD : (x + 1) * PAD, :]
    for (x_side, y_side), ref in zip(xy_sides, rho_xy):
        at_x = halo_start(x_side, cx, 0, WC + bx)
        at = pl.multiple_of(halo_start(y_side, cy, 0, PAD + BY), 8)
        block = ref[...].astype(F32)
        for x in range(WC):
            coarse[at_x + x, pl.ds(at, PAD), :] = block[x * PAD : (x + 1) * PAD, :]

    v0[...] = jnp.zeros_like(v0)
    v1[:, 0:PAD, :] = jnp.zeros((qx, PAD, LANES), F32)
    v1[:, ry - PAD : ry, :] = jnp.zeros((qx, PAD, LANES), F32)
    src[...] = jnp.zeros_like(src)
    for f, (ref, width) in enumerate(((v0, WV), (src, WS))):
        rows = f * fx * fy
        for x in range(fx):
            ref[WV + x, PAD : PAD + fy, :] = ext[rows + x * fy : rows + (x + 1) * fy, :]
        done = f * WV
        for side, got in zip(x_sides, fld_x):
            at = halo_start(side, cx, WV - width, WV + fx)
            for x in range(width):
                ref[at + x, PAD : PAD + fy, :] = got[(done + x) * fy : (done + x + 1) * fy, :].astype(F32)
        for side, got in zip(y_sides, fld_y):
            at = pl.multiple_of(halo_start(side, cy, 0, PAD + fy), 8)
            block = got[face_rows + f * fx * PAD : face_rows + (f + 1) * fx * PAD, :].astype(F32)
            for x in range(fx):
                ref[WV + x, pl.ds(at, PAD), :] = block[x * PAD : (x + 1) * PAD, :]
        for (x_side, y_side), got in zip(xy_sides, rho_xy):
            at_x = halo_start(x_side, cx, WV - width, WV + fx)
            at = pl.multiple_of(halo_start(y_side, cy, 0, PAD + fy), 8)
            block = got[(WC + 1) * PAD :, :].astype(F32)
            for x in range(width):
                ref[at_x + x, pl.ds(at, PAD), :] = block[(done + x) * PAD : (done + x + 1) * PAD, :]

    cells = (bx + 2 * WC) * rc
    wide[...] = wide_dot(coarse[...].reshape(cells, LANES), z_refine(cz))
    for p in range(bx + 2 * WC):
        base, half = p * rc + PAD // 2, ry // 2
        here = 0.75 * wide[pl.ds(base, half), :]
        fine[pl.ds(p * ry, half, stride=2), :] = here + 0.25 * wide[pl.ds(base - 1, half), :]
        fine[pl.ds(p * ry + 1, half, stride=2), :] = here + 0.25 * wide[pl.ds(base + 1, half), :]
    for q in range(1, qx - 1):
        at = q - WV
        here, other = at // 2 + WC, at // 2 + WC + (1 if at % 2 else -1)
        refined = 0.75 * fine[pl.ds(here * ry, ry), :] + 0.25 * fine[pl.ds(other * ry, ry), :]
        src[q] = math.pi * (refined - src[q])

    near, span = PAD - WS, fy + 2 * WS
    row = lax.broadcasted_iota(jnp.int32, (span, LANES), 0) - WS + fy * cy
    lane = lane_iota(span) - ZOFF + 2 * BZ * cz
    inside = (row >= 0) & (row < fy * counts[1]) & (lane >= 0) & (lane < 2 * BZ * counts[2])
    share = jnp.where(inside, 1.0 / 6.0, 0.0)
    old, new = v0, v1
    beside = z_neighbours()
    for sweep in range(SWEEPS):
        first, last = sweep + 1, qx - sweep - 1
        rows = old[first:last, near : near + span, :].reshape((last - first) * span, LANES)
        along_z = wide_dot(rows, beside)
        for q in range(first, last):
            at = q - WV + fx * cx
            total = along_z[(q - first) * span : (q - first + 1) * span]
            total = total + old[q - 1, near : near + span, :] + old[q + 1, near : near + span, :]
            total = total + old[q, near - 1 : near - 1 + span, :] + old[q, near + 1 : near + 1 + span, :]
            total = (total + src[q, near : near + span, :]) * share
            if q < WV or q >= WV + fx:
                total = jnp.where((at >= 0) & (at < fx * counts[0]), total, 0.0)
            new[q, near : near + span, :] = total
        old, new = new, old

    groups = fy // 4
    lane = lane_iota(groups)
    for x in range(fx):
        r = [old[WV + x, pl.ds(PAD + k, groups, stride=4), :] for k in range(4)]
        r1, r2 = pltpu.roll(r[1], 80, 1), pltpu.roll(r[2], 48, 1)
        potential[pl.ds(3 * groups * x, groups, stride=3), :] = jnp.where(lane < 96, pltpu.roll(r[0], 112, 1), r1)
        potential[pl.ds(3 * groups * x + 1, groups, stride=3), :] = jnp.where(lane < 64, r1, r2)
        potential[pl.ds(3 * groups * x + 2, groups, stride=3), :] = jnp.where(lane < 32, r2, pltpu.roll(r[3], 16, 1))

    send_potential = pltpu.make_async_copy(potential, potential_out, store_potential)
    send_potential.start()

    pieces = []
    for x in range(bx):
        q = WV + 2 * x
        fine[pl.ds(x * ry, ry), :] = 0.125 * (old[q - 1] + old[q + 2]) + 0.375 * (old[q] + old[q + 1])
        rows = [fine[pl.ds(x * ry + PAD + k, BY, stride=2), :] for k in (-1, 0, 1, 2)]
        pieces.append(0.125 * (rows[0] + rows[3]) + 0.375 * (rows[1] + rows[2]))
    back = wide_dot(jnp.concatenate(pieces, 0), z_coarsen())
    flat[...] = back
    for x, row in enumerate(merge_rows(flat, wide)):
        effective[x : x + 1, :] = row + local_part[x : x + 1, :]

    width, half = effective.shape[1], bands // 2
    lane = lane_iota(half)
    lane = jnp.concatenate([lane, lane], 0)
    spread = z_spread(cz)
    z_faces = mate_block[2 * potential.shape[0] :, :]
    step = 2 * LANES
    stores = []
    for j in range(0, width, step):
        columns = min(step, width - j)
        outer = jnp.dot(z_faces, spread[:, j : j + columns], preferred_element_type=F32)
        for x in range(bx):
            for t in range(j, j + columns, LANES):
                cut = slice(t, t + LANES)
                total = inner[x, :, cut] + effective[x : x + 1, cut] * orb[x, :, cut].astype(F32)
                total = total + outer[x * bands : (x + 1) * bands, t - j : t - j + LANES]
                for side, face in zip(y_sides, fld_y):
                    halo = -0.5 * face[x * half : (x + 1) * half, :].astype(F32)
                    if t == 0 and side != "hi":
                        here = jnp.concatenate([halo, pltpu.roll(halo, LANES - BZ, 1)], 0)
                        total = total + jnp.where((lane < BZ) & (cy > 0), here, 0.0)
                    if t == width - LANES and side != "lo":
                        here = [pltpu.roll(halo, LANES - BZ, 1), pltpu.roll(halo, LANES - 2 * BZ, 1)]
                        keep = (lane >= LANES - BZ) & (cy < counts[1] - 1)
                        total = total + jnp.where(keep, jnp.concatenate(here, 0), 0.0)
                for side, face in zip(x_sides, x_faces):
                    if x == 0 and side != "hi":
                        total = total + jnp.where(cx > 0, -0.5, 0.0) * face[:, cut].astype(F32)
                    if x == bx - 1 and side != "lo":
                        total = total + jnp.where(cx < counts[0] - 1, -0.5, 0.0) * face[:, cut].astype(F32)
                result[x, :, cut] = total.astype(BF16)
        cut = pl.ds(j, columns)
        stores.append(pltpu.make_async_copy(result.at[:, :, cut], out.at[:, :, cut], store.at[j // step]))
        stores[-1].start()
    for copy in stores + [send_potential]:
        copy.wait()


def laplace_kernel(orb, out):
    planes, bands, width = orb.shape
    step = 2 * LANES
    weights = [stencil(step * p % BZ, step) for p in range(3)]
    for j in range(0, width, step):
        columns = min(step, width - j)
        first, last = max(j - LANES, 0), min(j + step + LANES, width)
        skip = first - (j - LANES)
        w = weights[j // step % 3][skip : skip + last - first, :columns]
        here = orb[:, :, first:last].reshape(planes * bands, last - first)
        total = jnp.dot(here, w, preferred_element_type=F32).reshape(planes, bands, columns)
        for x in range(planes):
            near = [orb[n, :, j : j + columns].astype(F32) for n in (x - 1, x + 1) if 0 <= n < planes]
            out[x, :, j : j + columns] = total[x] - 0.5 * sum(near)


def vmem():
    return pl.BlockSpec(memory_space=pltpu.VMEM)


def local(mesh, orbitals, occupations, previous, compensation, local_potential):
    return step(mesh, orbitals, occupations, previous, compensation, local_potential)


def step(mesh, orbitals, occupations, previous, compensation, local_potential):
    domains, groups = mesh.shape["dom"], mesh.shape["band"]
    split_z = 2
    split_y = min(4, domains // 4)
    counts = (domains // (split_y * split_z), split_y, split_z)
    bands, _, bx, width = orbitals.shape
    tiles = width // LANES
    fx, fy = 2 * bx, 2 * BY
    x_sides, y_sides = sides(counts[0]), sides(counts[1])
    xy_sides = [(a, b) for a in x_sides for b in y_sides]
    moves = [{0: s} for s in x_sides] + [{1: s} for s in y_sides] + [{0: a, 1: b} for a, b in xy_sides]
    hbm = pl.BlockSpec(memory_space=pltpu.HBM)

    def shape(*dims, dtype=F32):
        return jax.ShapeDtypeStruct(dims, dtype)

    def params(kib):
        return pltpu.CompilerParams(vmem_limit_bytes=kib * 2**10)

    flat = [a.reshape(fx * fy * 2 * BZ // LANES, LANES) for a in (previous, compensation)]
    orb = jnp.transpose(orbitals.reshape(bands, bx, width), (1, 0, 2))
    mate_rows = 2 * flat[0].shape[0] + bx * bands
    inputs = [orb, occupations.reshape(1, bands), *flat]
    part, orb, mate_block, weight, *x_faces = pl.pallas_call(
        functools.partial(density_kernel, counts),
        in_specs=[hbm] * 4,
        out_specs=[vmem()] * (4 + len(x_sides)),
        out_shape=[shape(bx * tiles, LANES), shape(*orb.shape, dtype=BF16)]
        + [shape(mate_rows, LANES, dtype=BF16), shape(bands, LANES)]
        + [shape(bands, width, dtype=BF16) for _ in x_sides],
        scratch_shapes=[
            pltpu.VMEM((1, bands), F32),
            pltpu.VMEM((2, *flat[0].shape), F32),
            pltpu.SemaphoreType.DMA((bx,)),
            pltpu.SemaphoreType.DMA(()),
            pltpu.SemaphoreType.DMA((2,)),
        ],
        compiler_params=params(8 * 1024),
        name="density",
    )(*(pltpu.with_memory_space_constraint(a, pltpu.HBM) for a in inputs))
    x_faces = [fetch(f, counts, {0: s}) for s, f in zip(x_sides, x_faces)]
    mate_block = fetch(mate_block, counts, {2: "swap"})
    part = pl.pallas_call(
        strip_kernel,
        in_specs=[vmem()] * 3,
        out_specs=vmem(),
        out_shape=shape(bx * (tiles + 1), LANES),
        compiler_params=params(1024),
        name="strip",
    )(part, mate_block, weight)
    parts = [part]
    for shift in range(1, groups):
        route = [(i, i ^ shift if groups & (groups - 1) == 0 else (i + shift) % groups) for i in range(groups)]
        parts.append(lax.ppermute(part, "band", route))

    inner = pl.pallas_call(
        laplace_kernel,
        in_specs=[vmem()],
        out_specs=vmem(),
        out_shape=shape(bx, bands, width),
        compiler_params=params(16 * 1024),
        cost_estimate=pl.CostEstimate(flops=6 * 10**9, bytes_accessed=8 * 10**6, transcendentals=0),
        name="laplace",
    )(orb)

    rim_rows = [(WV + WS) * fy] * len(x_sides) + [bx * bands // 2 + 2 * fx * PAD] * len(y_sides)
    rim_rows += [(WV + WS + 1) * PAD] * len(xy_sides)
    ext, *rims = pl.pallas_call(
        functools.partial(field_kernel, counts),
        in_specs=[vmem()] * 4,
        out_specs=[vmem()] * (1 + len(rim_rows)),
        out_shape=[shape(2 * fx * fy, LANES)] + [shape(n, LANES, dtype=BF16) for n in rim_rows],
        scratch_shapes=[pltpu.VMEM((2 * flat[0].shape[0], LANES), F32)],
        compiler_params=params(4 * 1024),
        cost_estimate=pl.CostEstimate(flops=3 * 10**9, bytes_accessed=10**6, transcendentals=0),
        name="fields",
    )(orb, *flat, mate_block)
    corner_rims = rims[len(x_sides) + len(y_sides) :]
    fields = [fetch(r, counts, m) for r, m in zip(rims, moves) if list(m) == [0]]
    fields += [fetch(r, counts, m) for r, m in zip(rims, moves) if list(m) == [1]]

    corner_rows = (WC + 1) * PAD + (WV + WS + 1) * PAD
    cut_rows = [WC * BY] * len(x_sides) + [bx * PAD] * len(y_sides) + [corner_rows] * len(xy_sides)
    chip, *cuts = pl.pallas_call(
        functools.partial(total_kernel, counts, 1.0 / (bands * groups), groups),
        in_specs=[vmem()] * (groups + len(corner_rims)),
        out_specs=[vmem()] * (1 + len(cut_rows)),
        out_shape=[shape(bx * BY, LANES)] + [shape(n, LANES, dtype=BF16) for n in cut_rows],
        scratch_shapes=[pltpu.VMEM(part.shape, F32)],
        compiler_params=params(1024),
        name="total",
    )(*parts, *corner_rims)
    densities = [fetch(c, counts, m) for c, m in zip(cuts, moves)]

    rc, ry, qx = BY + 2 * PAD, fy + 2 * PAD, fx + 2 * WV
    local_rows = jnp.transpose(local_potential, (1, 0, 2))
    local_part = pl.pallas_call(
        functools.partial(local_kernel, counts),
        in_specs=[vmem(), vmem()],
        out_specs=vmem(),
        out_shape=shape(bx, width),
        scratch_shapes=[pltpu.VMEM((bx * BY, LANES), F32), pltpu.VMEM((bx * tiles, LANES), F32)],
        compiler_params=params(1024),
        name="local",
    )(chip, local_rows)
    operands = [chip, ext, local_part, orb, inner, mate_block, *densities, *fields, *x_faces]
    applied, potential = pl.pallas_call(
        functools.partial(finish_kernel, counts),
        in_specs=[vmem()] * len(operands),
        out_specs=[hbm, hbm],
        scratch_shapes=[
            pltpu.VMEM((bx + 2 * WC, rc, LANES), F32),
            pltpu.VMEM(((bx + 2 * WC) * rc, LANES), F32),
            pltpu.VMEM(((bx + 2 * WC) * ry, LANES), F32),
            pltpu.VMEM((qx, ry, LANES), F32),
            pltpu.VMEM((qx, ry, LANES), F32),
            pltpu.VMEM((qx, ry, LANES), F32),
            pltpu.VMEM((bx * BY, LANES), F32),
            pltpu.VMEM((bx, width), F32),
            pltpu.VMEM(flat[0].shape, F32),
            pltpu.VMEM((bx, bands, width), BF16),
            pltpu.SemaphoreType.DMA((pl.cdiv(width, 2 * LANES),)),
            pltpu.SemaphoreType.DMA(()),
        ],
        out_shape=[shape(bx, bands, width, dtype=BF16), shape(*flat[0].shape)],
        compiler_params=params(20 * 1024),
        name="finish",
    )(*operands)
    applied = jnp.transpose(applied, (1, 0, 2)).reshape(orbitals.shape)
    return applied, potential.reshape(previous.shape)


def solution(mesh):
    return jax.shard_map(
        functools.partial(local, mesh),
        mesh=mesh,
        in_specs=(
            P("band", "dom", None, None),
            P("band"),
            P("dom", None, None),
            P("dom", None, None),
            P("dom", None, None),
        ),
        out_specs=(P("band", "dom", None, None), P("dom", None, None)),
        check_vma=False,
    )
```
